32 devices in a mesh: parts: 2 (over y), leaf: 4 (over z), mid: 2 (over x), top: 2 (over core).
Axes of the slice: x: 2, y: 2, z: 4, core: 2. Of those that a mesh axis runs over, the one named last changes fastest.
Arguments:
- leaf_precision: float32 [8, 2, 2, 128, 128], P(('parts', 'leaf'), 'mid', 'top'), parts along dimension 0, may hold values from -40 to 40, as said below
- basis_fine: float32 [8, 2, 2, 128, 128], P(('parts', 'leaf'), 'mid', 'top'), parts along dimension 0, may hold values from -1 to 1
- basis_mid: float32 [8, 2, 2, 128, 128], P(('parts', 'leaf'), 'mid', 'top'), parts along dimension 0, may hold values from -1 to 1
- basis_coarse: float32 [8, 2, 2, 128, 128], P(('parts', 'leaf'), 'mid', 'top'), parts along dimension 0, may hold values from -1 to 1
- core_fine: float32 [128, 128], replicated, may hold values from -20 to 20, as said below
- core_mid: float32 [128, 128], replicated, may hold values from -20 to 20, as said below
- core_coarse: float32 [128, 128], replicated, may hold values from -20 to 20, as said below
- observations: float32 [8, 2, 2, 128, 128], P(('parts', 'leaf'), 'mid', 'top'), parts along dimension 0, may hold values from -20 to 20
Outputs:
- solution: float32 [8, 2, 2, 128, 128], P(('parts', 'leaf'), 'mid', 'top'), parts along dimension 0
The draws below stay inside these ranges and needn't reach their ends.
There are 2 independent parts, one for each index of `parts`. The reference program is written for one: setup_inputs(seed, part) draws one part's arguments, and reference() takes and returns one part's arrays. A program takes and returns all parts, laid end to end along the dimension named above; an argument that names none is the same for every part. Nothing has to cross between parts.
Inputs may be any that keep to these rules, and one draw needn't show every extreme that they name: Every leaf_precision[l, m, t] is symmetric positive definite. `core_fine`: symmetric positive definite. `core_mid`: symmetric positive definite. `core_coarse`: symmetric positive definite.
All inputs are finite; a program needn't handle non-finite values.
Results may differ from the reference program's by a relative error of at most 0.00005.
Values sent between devices are 32-bit elements; how exact they have to be, the bound alone decides.
A program may use at most 64 MiB of HBM per device.

```python
import jax
import jax.numpy as jnp
from jax import lax

ROWS = 128
R = 128
COLS = 128
GROUP_FINE = 512
GROUP_MID = 1024
POINTS = 2048
N_LEAF = 4
N_MID = 2
N_TOP = 2


def log_between(key, shape, lower, upper):
    return jnp.exp(jax.random.uniform(key, shape, jnp.float32, jnp.log(lower), jnp.log(upper)))


def draw_leaf_precision(key, part):
    key_mix, key_diag = jax.random.split(jax.random.fold_in(key, 1), 2)
    shape = (N_LEAF, N_MID, N_TOP, ROWS, ROWS)
    mixing = jax.random.normal(key_mix, shape, jnp.float32) / jnp.sqrt(jnp.float32(ROWS))
    product = jnp.einsum('lmtij,lmtkj->lmtik', mixing, mixing, precision=lax.Precision.HIGHEST)
    diagonal = log_between(key_diag, shape[:-1], 0.5, 2.0)
    eye_rows = jnp.eye(ROWS, dtype=jnp.float32)
    result = 0.5 * product + diagonal[..., :, None] * eye_rows
    return result


def core_matrix(key, salt):
    key_mix, key_diag = jax.random.split(jax.random.fold_in(key, salt), 2)
    mixing = jax.random.normal(key_mix, (R, R), jnp.float32)
    product = jnp.dot(mixing, mixing.T, precision=lax.Precision.HIGHEST) / R
    diagonal = log_between(key_diag, (R,), 0.5, 2.0)
    result = 0.3 * product + jnp.diag(diagonal)
    return result


def draw_core_fine(key, part):
    return core_matrix(key, 11)


def draw_core_mid(key, part):
    return core_matrix(key, 12)


def draw_core_coarse(key, part):
    return core_matrix(key, 13)


def basis_level(key, salt, group_rows):
    key_entry = jax.random.fold_in(jax.random.fold_in(key, salt), 0)
    shape = (N_LEAF, N_MID, N_TOP, ROWS, R)
    entries = jnp.clip(jax.random.normal(key_entry, shape, jnp.float32), -5.0, 5.0)
    return entries / jnp.sqrt(jnp.float32(group_rows))


def draw_basis_fine(key, part):
    return basis_level(key, 101, GROUP_FINE)


def draw_basis_mid(key, part):
    return basis_level(key, 102, GROUP_MID)


def draw_basis_coarse(key, part):
    return basis_level(key, 103, POINTS)


def draw_observations(key, part):
    precise = lax.Precision.HIGHEST
    fine_basis = basis_level(key, 101, GROUP_FINE)
    mid_basis = basis_level(key, 102, GROUP_MID)
    coarse_basis = basis_level(key, 103, POINTS)
    key_fine, key_mid, key_coarse, key_noise = jax.random.split(jax.random.fold_in(key, 200), 4)
    fine_weight = jnp.clip(jax.random.normal(key_fine, (N_MID, N_TOP, R, COLS), jnp.float32), -5.0, 5.0) * (0.7 * jnp.sqrt(jnp.float32(GROUP_FINE) / R))
    mid_weight = jnp.clip(jax.random.normal(key_mid, (N_TOP, R, COLS), jnp.float32), -5.0, 5.0) * (0.7 * jnp.sqrt(jnp.float32(GROUP_MID) / R))
    coarse_weight = jnp.clip(jax.random.normal(key_coarse, (R, COLS), jnp.float32), -5.0, 5.0) * (0.7 * jnp.sqrt(jnp.float32(POINTS) / R))
    noise = jnp.clip(jax.random.normal(key_noise, (N_LEAF, N_MID, N_TOP, ROWS, COLS), jnp.float32), -5.0, 5.0)
    signal = jnp.einsum('lmtrk,mtkc->lmtrc', fine_basis, fine_weight, precision=precise)
    signal = signal + jnp.einsum('lmtrk,tkc->lmtrc', mid_basis, mid_weight, precision=precise)
    signal = signal + jnp.einsum('lmtrk,kc->lmtrc', coarse_basis, coarse_weight, precision=precise)
    return jnp.clip(signal + noise, -20.0, 20.0)


def setup_inputs(seed: int = 0, part: int = 0) -> dict:
    splits = jax.random.split(jax.random.key(seed), 9)
    part_keys = jax.random.split(jax.random.fold_in(splits[8], part), 9)
    return {
        "leaf_precision": draw_leaf_precision(jax.random.fold_in(jax.random.fold_in(splits[8], part), 71), part),
        "basis_fine": draw_basis_fine(jax.random.fold_in(jax.random.fold_in(splits[8], part), 71), part),
        "basis_mid": draw_basis_mid(jax.random.fold_in(jax.random.fold_in(splits[8], part), 71), part),
        "basis_coarse": draw_basis_coarse(jax.random.fold_in(jax.random.fold_in(splits[8], part), 71), part),
        "core_fine": draw_core_fine(jax.random.fold_in(splits[8], 71), part),
        "core_mid": draw_core_mid(jax.random.fold_in(splits[8], 71), part),
        "core_coarse": draw_core_coarse(jax.random.fold_in(splits[8], 71), part),
        "observations": draw_observations(jax.random.fold_in(jax.random.fold_in(splits[8], part), 71), part),
    }


def solve_core(matrix, right_side):
    return jax.scipy.linalg.cho_solve((jnp.linalg.cholesky(matrix), True), right_side)

def batched_solve(matrix, right_side):
    lead = matrix.shape[:-2]
    flat_matrix = matrix.reshape((-1,) + matrix.shape[-2:])
    flat_right = right_side.reshape((-1,) + right_side.shape[-2:])
    result = jax.vmap(solve_core)(flat_matrix, flat_right)
    return result.reshape(lead + right_side.shape[-2:])

def reference(leaf_precision, basis_fine, basis_mid, basis_coarse, core_fine, core_mid, core_coarse, observations):
    precise = lax.Precision.HIGHEST
    core_rank = basis_fine.shape[4]
    stacked = jnp.concatenate([basis_fine, basis_mid, basis_coarse, observations], axis=4)
    solved = jnp.einsum('lmtij,lmtjc->lmtic', leaf_precision, stacked, precision=precise)
    fine_gram = jnp.einsum('lmtrk,lmtrc->mtkc', basis_fine, solved, precision=precise)
    fine_coef = batched_solve(core_fine[None, None] + fine_gram[..., :core_rank], fine_gram[..., core_rank:])
    after_fine = solved[..., core_rank:] - jnp.einsum('lmtrk,mtkc->lmtrc', solved[..., :core_rank], fine_coef, precision=precise)
    mid_gram = jnp.einsum('lmtrk,lmtrc->tkc', basis_mid, after_fine, precision=precise)
    mid_coef = batched_solve(core_mid[None] + mid_gram[..., :core_rank], mid_gram[..., core_rank:])
    after_mid = after_fine[..., core_rank:] - jnp.einsum('lmtrk,tkc->lmtrc', after_fine[..., :core_rank], mid_coef, precision=precise)
    coarse_gram = jnp.einsum('lmtrk,lmtrc->kc', basis_coarse, after_mid, precision=precise)
    coarse_coef = solve_core(core_coarse + coarse_gram[:, :core_rank], coarse_gram[:, core_rank:])
    return after_mid[..., core_rank:] - jnp.einsum('lmtrk,kc->lmtrc', after_mid[..., :core_rank], coarse_coef, precision=precise)
```

```python
import functools

import jax
import jax.numpy as jnp
from jax import lax
from jax.experimental import pallas as pl
from jax.experimental.pallas import tpu as pltpu
from jax.sharding import PartitionSpec as P

MESH = pl.DeviceIdType.MESH
PANEL = 8


def dot(left_hand, right_side):
    return jnp.dot(
        left_hand, right_side, precision=lax.Precision.HIGHEST, preferred_element_type=jnp.float32
    )


def split3(x):
    high = x.astype(jnp.bfloat16).astype(jnp.float32)
    rest = x - high
    mid = rest.astype(jnp.bfloat16).astype(jnp.float32)
    low = (rest - mid).astype(jnp.bfloat16).astype(jnp.float32)
    return high, mid, low


def spread_panel(panel):
    p1, p2, p3 = split3(panel)
    return jnp.concatenate([p1, p1, p2, p2, p1, p3], axis=0).T.astype(jnp.bfloat16)


def rank_update(spread, scaled):
    r1, r2, r3 = split3(scaled)
    right_side = jnp.concatenate([r1, r2, r1, r2, r3, r1], axis=0).astype(jnp.bfloat16)
    return jnp.dot(spread, right_side, preferred_element_type=jnp.float32)


def negated_inverse(a_ref, matrix):
    size = matrix.shape[0]
    zero = jnp.zeros((PANEL, size), jnp.float32)
    a_ref[pl.ds(0, PANEL), :] = zero
    a_ref[pl.ds(PANEL, size), :] = matrix
    a_ref[pl.ds(PANEL + size, PANEL), :] = zero
    lane = lax.broadcasted_iota(jnp.int32, (PANEL, size), 1)
    sub = lax.broadcasted_iota(jnp.int32, (PANEL, size), 0)
    lane_full = lax.broadcasted_iota(jnp.int32, (size, size), 1)

    def columns(block, k):
        return [
            jnp.broadcast_to(
                jnp.sum(jnp.where(lane == k * PANEL + j, block, 0.0), axis=1, keepdims=True),
                block.shape,
            )
            for j in range(PANEL)
        ]

    def apply(k, spread, scaled):
        inside = (lane_full >= k * PANEL) & (lane_full < (k + 1) * PANEL)
        current = a_ref[pl.ds(PANEL, size), :]
        a_ref[pl.ds(PANEL, size), :] = jnp.where(inside, 0.0, current) - rank_update(spread, scaled)
        a_ref[pl.ds(pl.multiple_of((k + 1) * PANEL, PANEL), PANEL), :] = scaled

    def body(k, carry):
        spread_before, scaled_before, panel = carry
        apply(k - 1, spread_before, scaled_before)
        spread = spread_panel(panel)
        inside = (lane >= k * PANEL) & (lane < (k + 1) * PANEL)
        cols = columns(panel, k)
        ahead = lane == (k + 1) * PANEL + sub
        coefs = [
            jnp.broadcast_to(
                jnp.sum(
                    jnp.where(ahead, jnp.broadcast_to(panel[j : j + 1], panel.shape), 0.0),
                    axis=1, keepdims=True,
                ),
                panel.shape,
            )
            for j in range(PANEL)
        ]
        x = jnp.where(inside, jnp.where(lane - k * PANEL == sub, 1.0, 0.0), panel)
        for i in range(PANEL):
            pivot = 1.0 / jnp.broadcast_to(cols[i][i : i + 1], x.shape)
            here = sub == i

            def step(v):
                row = jnp.broadcast_to(v[i : i + 1], v.shape) * pivot
                return jnp.where(here, row, v - cols[i] * row)

            x_new = step(x)
            for j in range(i + 1, PANEL):
                cols[j] = step(cols[j])
            x = x_new
        scaled = jnp.where(inside, -x, x)
        following = a_ref[pl.ds(pl.multiple_of((k + 2) * PANEL, PANEL), PANEL), :]
        panel_next = jnp.where(inside, 0.0, following)
        for j in range(PANEL):
            panel_next = panel_next - coefs[j] * jnp.broadcast_to(scaled[j : j + 1], x.shape)
        return spread, scaled, panel_next

    steps = size // PANEL
    spread, scaled, _ = lax.fori_loop(0, steps, body, (spread_panel(zero), zero, matrix[:PANEL]))
    apply(steps - 1, spread, scaled)
    return a_ref[pl.ds(PANEL, size), :]


def dot_nt(left_hand, right_rows):
    return lax.dot_general(
        left_hand, right_rows, (((1,), (1,)), ((), ())),
        precision=lax.Precision.HIGHEST, preferred_element_type=jnp.float32,
    )


def pack(matrix):
    half, size = matrix.shape[0] // 2, matrix.shape[1]
    lane = lax.broadcasted_iota(jnp.int32, (half, size), 1)
    row = lax.broadcasted_iota(jnp.int32, (half, size), 0)
    bottom = pltpu.roll(matrix[half:], half, 1)
    main = jnp.where(lane < row, bottom, matrix[:half])
    diagonal = jnp.sum(jnp.where(lane == row, bottom, 0.0), axis=0, keepdims=True)
    return main, jnp.broadcast_to(diagonal, (PANEL, size))


def unpack(main, diagonal):
    half, size = main.shape
    lane = lax.broadcasted_iota(jnp.int32, (half, size), 1)
    row = lax.broadcasted_iota(jnp.int32, (half, size), 0)
    flipped = jnp.concatenate([main, main], axis=0).T
    top = jnp.where(lane < row, flipped[:half], main)
    lower = jnp.where(lane < row, main, flipped[:half])
    lower = jnp.where(lane == row, jnp.broadcast_to(diagonal[:1], lower.shape), lower)
    bottom = jnp.where(lane < half, flipped[half:], pltpu.roll(lower, half, 1))
    return jnp.concatenate([top, bottom], axis=0)


FF, MF, MM, CF, CM, CC, YF, YM, YC = range(9)
SYMMETRIC = (FF, MM, CC)


def kernel(
    n_leaf, n_mid, n_top,
    prec_hbm, fine_hbm, mid_hbm, coarse_hbm, core_fine_hbm, core_mid_hbm, core_coarse_hbm, obs_hbm,
    out_ref,
    in_ref, a_ref, s_ref, bulk_ref, gram_in, pass_ref, total_ref, fine_ref, mid_ref, cross_ref, cross_in, last_ref,
    in_sem, gram_send, gram_recv, fine_send, fine_recv, mid_send, mid_recv, cross_send, cross_recv, last_send, last_recv,
):
    r = bulk_ref.shape[1]
    packed = r // 2 + PANEL
    leaf, mid, top = lax.axis_index("leaf"), lax.axis_index("mid"), lax.axis_index("top")

    def root_of(index):
        return (n_leaf - 1) // 2 + lax.rem(index, 2) * (n_leaf // 2 - (n_leaf - 1) // 2)

    root = root_of(top)
    is_root = leaf == root
    is_other = leaf != root
    barrier = pltpu.get_barrier_semaphore()

    def greet(device):
        pl.semaphore_signal(barrier, inc=1, device_id=device, device_id_type=MESH)

    leaf_steps = sorted(range(1, n_leaf), key=lambda step: (abs(2 * step - n_leaf), step))

    def along(axis, index, count, step):
        return {axis: lax.rem(index + step, count)}

    for t in range(n_top):
        @pl.when((leaf != root_of(t)) | (top != t))
        def _():
            greet({"leaf": root_of(t), "top": jnp.int32(t)})

    @pl.when(is_root)
    def _():
        for step in leaf_steps:
            greet(along("leaf", leaf, n_leaf, step))
        for step in range(1, n_mid):
            greet(along("mid", mid, n_mid, step))

    sources = [prec_hbm, fine_hbm, mid_hbm, coarse_hbm, obs_hbm, core_fine_hbm, core_mid_hbm, core_coarse_hbm]
    loads = [pltpu.make_async_copy(src, in_ref.at[k], in_sem.at[k]) for k, src in enumerate(sources)]
    for load in loads:
        load.start()

    def fetch(k):
        loads[k].wait()
        return in_ref[k]

    def rows(block):
        return slice(0, packed if block in SYMMETRIC else r)

    def gram_copy(block, slot):
        return pltpu.make_async_remote_copy(
            src_ref=bulk_ref.at[block, rows(block)], dst_ref=gram_in.at[slot, block, rows(block)],
            send_sem=gram_send.at[block], recv_sem=gram_recv.at[slot, block],
            device_id={"leaf": root}, device_id_type=MESH,
        )

    slot_here = lax.rem(root - leaf + n_leaf, n_leaf) - 1

    def store(ref, block, value, symmetric):
        if symmetric:
            main, diagonal = pack(value)
            ref[block, : r // 2] = main
            ref[block, r // 2 : packed] = diagonal
        else:
            ref[block] = value

    def hand_in(block, value):
        store(bulk_ref, block, value, block in SYMMETRIC)

        @pl.when(is_other)
        def _():
            gram_copy(block, slot_here).start()

    prec, fine = fetch(0), fetch(1)
    solved_f = dot(prec, fine)
    s_ref[0] = solved_f
    gram_ff = dot(fine.T, solved_f)

    @pl.when(is_root)
    def _():
        pl.semaphore_wait(barrier, n_leaf * n_top - 1 + n_mid - 1)

    @pl.when(is_other)
    def _():
        pl.semaphore_wait(barrier, 1)

    hand_in(FF, gram_ff)
    middle = fetch(2)
    mid_t = middle.T
    hand_in(MF, dot(mid_t, solved_f))
    solved_m = dot(prec, middle)
    s_ref[1] = solved_m
    hand_in(MM, dot(mid_t, solved_m))
    coarse = fetch(3)
    coarse_t = coarse.T
    hand_in(CF, dot(coarse_t, solved_f))
    hand_in(CM, dot(coarse_t, solved_m))
    solved_c = dot(prec, coarse)
    s_ref[2] = solved_c
    hand_in(CC, dot(coarse_t, solved_c))
    obs = fetch(4)
    obs_t = obs.T
    hand_in(YF, dot(obs_t, solved_f))
    hand_in(YM, dot(obs_t, solved_m))
    hand_in(YC, dot(obs_t, solved_c))
    s_ref[3] = dot(prec, obs)
    for k in range(5, 8):
        loads[k].wait()

    def spread(ref, sends, recvs, block, step):
        return pltpu.make_async_remote_copy(
            src_ref=ref.at[block], dst_ref=ref.at[block],
            send_sem=sends.at[block, step - 1], recv_sem=recvs.at[block],
            device_id=along("leaf", leaf, n_leaf, step), device_id_type=MESH,
        )

    def cross_copy(block, step):
        place = slice(0, packed if block in (0, 3) else r)
        return pltpu.make_async_remote_copy(
            src_ref=cross_ref.at[block, place], dst_ref=cross_in.at[step - 1, block, place],
            send_sem=cross_send.at[block, step - 1], recv_sem=cross_recv.at[block, step - 1],
            device_id=along("mid", mid, n_mid, step), device_id_type=MESH,
        )

    others = [(a, b) for a in [*leaf_steps, 0] for b in reversed(range(n_top)) if (a, b) != (0, 0)]

    def last_copy(block, source, number):
        a, b = others[number]
        place = slice(0, packed if block == 0 else r)
        return pltpu.make_async_remote_copy(
            src_ref=last_ref.at[source, block, place], dst_ref=last_ref.at[source, block, place],
            send_sem=last_send.at[block, number], recv_sem=last_recv.at[block, source],
            device_id={**along("leaf", leaf, n_leaf, a), **along("top", top, n_top, b)}, device_id_type=MESH,
        )

    def gathered(block):
        place = rows(block)
        total = bulk_ref[block, place]
        for slot in range(n_leaf - 1):
            gram_copy(block, slot).wait_recv()
            total = total + gram_in[slot, block, place]
        return total

    def whole(value):
        return unpack(value[: r // 2], value[r // 2 :])

    def cross_send_off(block, value, symmetric):
        store(cross_ref, block, value, symmetric)
        for step in range(1, n_mid):
            cross_copy(block, step).start()

    def crossed(block):
        place = slice(0, packed if block in (0, 3) else r)
        total = cross_ref[block, place]
        for step in range(1, n_mid):
            cross_copy(block, step).wait_recv()
            total = total + cross_in[step - 1, block, place]
        return total

    @pl.when(is_root)
    def _():
        inverse = negated_inverse(a_ref, in_ref[5] + whole(gathered(FF)))
        mf = gathered(MF)
        n_m = dot(mf, inverse)
        cross_send_off(0, whole(gathered(MM)) + dot_nt(n_m, mf), True)
        fine_ref[0] = n_m
        cf = gathered(CF)
        n_c = dot(cf, inverse)
        cross_send_off(1, gathered(CM) + dot_nt(n_c, mf), False)
        cross_send_off(3, whole(gathered(CC)) + dot_nt(n_c, cf), True)
        fine_ref[1] = n_c
        total_ref[0] = inverse
        total_ref[1] = mf
        total_ref[2] = cf
        for block in range(2):
            for step in leaf_steps:
                spread(fine_ref, fine_send, fine_recv, block, step).start()

        inverse = negated_inverse(a_ref, in_ref[6] + whole(crossed(0)))
        cm = crossed(1)
        q_c = dot(cm, inverse)
        store(last_ref.at[top], 0, whole(crossed(3)) + dot_nt(q_c, cm), True)
        for number in range(len(others)):
            last_copy(0, top, number).start()
        mid_ref[0] = q_c

        n_y = dot(gathered(YF), total_ref[0])
        cross_send_off(2, gathered(YM) + dot_nt(n_y, total_ref[1]), False)
        cross_send_off(4, gathered(YC) + dot_nt(n_y, total_ref[2]), False)
        fine_ref[2] = n_y
        for step in leaf_steps:
            spread(mid_ref, mid_send, mid_recv, 0, step).start()
            spread(fine_ref, fine_send, fine_recv, 2, step).start()
        q_y = dot(crossed(2), inverse)
        last_ref[top, 1] = crossed(4) + dot_nt(q_y, cm)
        for number in range(len(others)):
            last_copy(1, top, number).start()
        mid_ref[1] = q_y
        for step in leaf_steps:
            spread(mid_ref, mid_send, mid_recv, 1, step).start()

    def arrived(block):
        for t in range(n_top):
            @pl.when(is_other | (top != t))
            def _():
                last_copy(block, t, 0).wait_recv()

    arrived(0)
    coarse_sum = last_ref[0, 0, :packed]
    for t in range(1, n_top):
        coarse_sum = coarse_sum + last_ref[t, 0, :packed]
    inverse = negated_inverse(a_ref, in_ref[7] + whole(coarse_sum))

    @pl.when(is_other)
    def _():
        for block in range(3):
            spread(fine_ref, fine_send, fine_recv, block, 1).wait_recv()
        for block in range(2):
            spread(mid_ref, mid_send, mid_recv, block, 1).wait_recv()

    solved_f = s_ref[0]
    after_m = s_ref[1] + dot_nt(solved_f, fine_ref[0])
    after_c = s_ref[2] + dot_nt(solved_f, fine_ref[1]) + dot_nt(after_m, mid_ref[0])
    after_y = s_ref[3] + dot_nt(solved_f, fine_ref[2]) + dot_nt(after_m, mid_ref[1])
    arrived(1)
    right = last_ref[0, 1]
    for t in range(1, n_top):
        right = right + last_ref[t, 1]
    out_ref[...] = after_y + dot_nt(after_c, dot(right, inverse))

    @pl.when(is_root)
    def _():
        for block in range(5):
            for step in range(1, n_mid):
                cross_copy(block, step).wait_send()
        for step in leaf_steps:
            for block in range(3):
                spread(fine_ref, fine_send, fine_recv, block, step).wait_send()
            for block in range(2):
                spread(mid_ref, mid_send, mid_recv, block, step).wait_send()
        for block in range(2):
            for number in range(len(others)):
                last_copy(block, top, number).wait_send()

    @pl.when(is_other)
    def _():
        for block in range(9):
            gram_copy(block, slot_here).wait_send()


def local(n_leaf, n_mid, n_top, *operands):
    blocks = [x.reshape(x.shape[-2:]) for x in operands]
    r = blocks[1].shape[1]
    f32 = jnp.float32
    dma = pltpu.SemaphoreType.DMA
    answer = pl.pallas_call(
        functools.partial(kernel, n_leaf, n_mid, n_top),
        out_shape=jax.ShapeDtypeStruct(blocks[-1].shape, f32),
        in_specs=[pl.BlockSpec(memory_space=pl.ANY)] * len(blocks),
        out_specs=pl.BlockSpec(memory_space=pltpu.VMEM),
        scratch_shapes=[
            pltpu.VMEM((8, r, r), f32),
            pltpu.VMEM((r + 2 * PANEL, r), f32),
            pltpu.VMEM((4, r, r), f32),
            pltpu.VMEM((9, r, r), f32),
            pltpu.VMEM((n_leaf - 1, 9, r, r), f32),
            pltpu.VMEM((PANEL, r), f32),
            pltpu.VMEM((3, r, r), f32),
            pltpu.VMEM((3, r, r), f32),
            pltpu.VMEM((2, r, r), f32),
            pltpu.VMEM((5, r, r), f32),
            pltpu.VMEM((n_mid - 1, 5, r, r), f32),
            pltpu.VMEM((n_top, 2, r, r), f32),
            dma((8,)),
            dma((9,)), dma((n_leaf - 1, 9)),
            dma((3, n_leaf - 1)), dma((3,)),
            dma((2, n_leaf - 1)), dma((2,)),
            dma((5, n_mid - 1)), dma((5, n_mid - 1)),
            dma((2, n_leaf * n_top - 1)), dma((2, n_top)),
        ],
        compiler_params=pltpu.CompilerParams(collective_id=0, has_side_effects=True),
    )(*blocks)
    return answer[None, None, None]


def solution(mesh):
    spread = P(("parts", "leaf"), "mid", "top", None, None)
    sizes = (mesh.shape["leaf"], mesh.shape["mid"], mesh.shape["top"])
    return jax.shard_map(
        functools.partial(local, *sizes),
        mesh=mesh,
        in_specs=(spread, spread, spread, spread, P(), P(), P(), spread),
        out_specs=spread,
        check_vma=False,
    )
```

```python
import functools

import jax
import jax.numpy as jnp
from jax import lax
from jax.experimental import pallas as pl
from jax.experimental.pallas import tpu as pltpu
from jax.sharding import PartitionSpec as P

MESH = pl.DeviceIdType.MESH
PANEL = 8


def dot(left_hand, right_side):
    return jnp.dot(
        left_hand, right_side, precision=lax.Precision.HIGHEST, preferred_element_type=jnp.float32
    )


def split3(x):
    high = x.astype(jnp.bfloat16).astype(jnp.float32)
    rest = x - high
    mid = rest.astype(jnp.bfloat16).astype(jnp.float32)
    low = (rest - mid).astype(jnp.bfloat16).astype(jnp.float32)
    return high, mid, low


def spread_panel(panel):
    p1, p2, p3 = split3(panel)
    return jnp.concatenate([p1, p1, p2, p2, p1, p3], axis=0).T.astype(jnp.bfloat16)


def rank_update(spread, scaled):
    r1, r2, r3 = split3(scaled)
    right_side = jnp.concatenate([r1, r2, r1, r2, r3, r1], axis=0).astype(jnp.bfloat16)
    return jnp.dot(spread, right_side, preferred_element_type=jnp.float32)


def negated_inverse(a_ref, matrix, between=None):
    size = matrix.shape[0]
    zero = jnp.zeros((PANEL, size), jnp.float32)
    a_ref[pl.ds(0, PANEL), :] = zero
    a_ref[pl.ds(PANEL, size), :] = matrix
    a_ref[pl.ds(PANEL + size, PANEL), :] = zero
    lane = lax.broadcasted_iota(jnp.int32, (PANEL, size), 1)
    sub = lax.broadcasted_iota(jnp.int32, (PANEL, size), 0)
    lane_full = lax.broadcasted_iota(jnp.int32, (size, size), 1)

    def columns(block, k):
        return [
            jnp.broadcast_to(
                jnp.sum(jnp.where(lane == k * PANEL + j, block, 0.0), axis=1, keepdims=True),
                block.shape,
            )
            for j in range(PANEL)
        ]

    def apply(k, spread, scaled):
        inside = (lane_full >= k * PANEL) & (lane_full < (k + 1) * PANEL)
        current = a_ref[pl.ds(PANEL, size), :]
        a_ref[pl.ds(PANEL, size), :] = jnp.where(inside, 0.0, current) - rank_update(spread, scaled)
        a_ref[pl.ds(pl.multiple_of((k + 1) * PANEL, PANEL), PANEL), :] = scaled

    def body(k, carry):
        spread_before, scaled_before, panel = carry
        apply(k - 1, spread_before, scaled_before)
        spread = spread_panel(panel)
        inside = (lane >= k * PANEL) & (lane < (k + 1) * PANEL)
        cols = columns(panel, k)
        ahead = lane == (k + 1) * PANEL + sub
        coefs = [
            jnp.broadcast_to(
                jnp.sum(
                    jnp.where(ahead, jnp.broadcast_to(panel[j : j + 1], panel.shape), 0.0),
                    axis=1, keepdims=True,
                ),
                panel.shape,
            )
            for j in range(PANEL)
        ]
        x = jnp.where(inside, jnp.where(lane - k * PANEL == sub, 1.0, 0.0), panel)
        for i in range(PANEL):
            pivot = 1.0 / jnp.broadcast_to(cols[i][i : i + 1], x.shape)
            here = sub == i

            def step(v):
                row = jnp.broadcast_to(v[i : i + 1], v.shape) * pivot
                return jnp.where(here, row, v - cols[i] * row)

            x_new = step(x)
            for j in range(i + 1, PANEL):
                cols[j] = step(cols[j])
            x = x_new
        scaled = jnp.where(inside, -x, x)
        following = a_ref[pl.ds(pl.multiple_of((k + 2) * PANEL, PANEL), PANEL), :]
        panel_next = jnp.where(inside, 0.0, following)
        for j in range(PANEL):
            panel_next = panel_next - coefs[j] * jnp.broadcast_to(scaled[j : j + 1], x.shape)
        return spread, scaled, panel_next

    steps = size // PANEL
    carry = (spread_panel(zero), zero, matrix[:PANEL])
    if between is None:
        spread, scaled, _ = lax.fori_loop(0, steps, body, carry)
    else:
        carry = lax.fori_loop(0, steps // 2, body, carry)
        between()
        spread, scaled, _ = lax.fori_loop(steps // 2, steps, body, carry)
    apply(steps - 1, spread, scaled)
    return a_ref[pl.ds(PANEL, size), :]


def dot_nt(left_hand, right_rows):
    return lax.dot_general(
        left_hand, right_rows, (((1,), (1,)), ((), ())),
        precision=lax.Precision.HIGHEST, preferred_element_type=jnp.float32,
    )


def pack(matrix):
    half, size = matrix.shape[0] // 2, matrix.shape[1]
    lane = lax.broadcasted_iota(jnp.int32, (half, size), 1)
    row = lax.broadcasted_iota(jnp.int32, (half, size), 0)
    bottom = pltpu.roll(matrix[half:], half, 1)
    main = jnp.where(lane < row, bottom, matrix[:half])
    diagonal = jnp.sum(jnp.where(lane == row, bottom, 0.0), axis=0, keepdims=True)
    return main, jnp.broadcast_to(diagonal, (PANEL, size))


def unpack(main, diagonal):
    half, size = main.shape
    lane = lax.broadcasted_iota(jnp.int32, (half, size), 1)
    row = lax.broadcasted_iota(jnp.int32, (half, size), 0)
    flipped = jnp.concatenate([main, main], axis=0).T
    top = jnp.where(lane < row, flipped[:half], main)
    lower = jnp.where(lane < row, main, flipped[:half])
    lower = jnp.where(lane == row, jnp.broadcast_to(diagonal[:1], lower.shape), lower)
    bottom = jnp.where(lane < half, flipped[half:], pltpu.roll(lower, half, 1))
    return jnp.concatenate([top, bottom], axis=0)


FF, MF, MM, CF, CM, YF, YM, CC, YC = range(9)
SYMMETRIC = (FF, MM)
LATER = (CM, CC, YF, YM, YC)
PIECES = (CM, YM, CC, YC)


def kernel(
    n_leaf, n_mid, n_top,
    prec_hbm, fine_hbm, mid_hbm, coarse_hbm, core_fine_hbm, core_mid_hbm, core_coarse_hbm, obs_hbm,
    out_ref,
    in_ref, a_ref, s_ref, raw_ref, bulk_ref, piece_in, gram_in, total_ref, down_ref, cross_ref, cross_in, last_ref,
    in_sem, piece_send, piece_recv, gram_send, gram_recv, down_send, down_recv,
    cross_send, cross_recv, last_send, last_recv, swap_send,
):
    r = bulk_ref.shape[1]
    packed = r // 2 + PANEL
    leaf, mid, top = lax.axis_index("leaf"), lax.axis_index("mid"), lax.axis_index("top")
    low, high = (n_leaf - 1) // 2, n_leaf // 2
    root = low + lax.rem(top, 2) * (high - low)
    is_root = leaf == root
    is_other = leaf != root
    side = (leaf > root).astype(jnp.int32)
    inner, outer = leaf + 1 - 2 * side, leaf - 1 + 2 * side
    has_outer = is_other & (outer >= 0) & (outer < n_leaf)
    inner_is_other = is_other & (inner != root)
    barrier = pltpu.get_barrier_semaphore()

    def greet(device):
        pl.semaphore_signal(barrier, inc=1, device_id=device, device_id_type=MESH)

    leaf_steps = sorted(range(1, n_leaf), key=lambda step: (abs(2 * step - n_leaf), step))
    peers = [(a, b) for a in range(n_mid) for b in range(n_top) if (a, b) != (0, 0)]

    def beside(a, b):
        return {"mid": lax.rem(mid + a, n_mid), "top": lax.rem(top + b, n_top)}

    def leaf_at(step):
        return {"leaf": lax.rem(leaf + step, n_leaf)}

    for a, b in peers:
        greet(beside(a, b))

    @pl.when(is_root)
    def _():
        for step in leaf_steps:
            greet(leaf_at(step))

    @pl.when(is_other)
    def _():
        greet({"leaf": root})

    @pl.when(has_outer)
    def _():
        greet({"leaf": outer})

    @pl.when(inner_is_other)
    def _():
        greet({"leaf": inner})

    sources = [prec_hbm, fine_hbm, mid_hbm, coarse_hbm, obs_hbm, core_fine_hbm, core_mid_hbm, core_coarse_hbm]
    loads = [pltpu.make_async_copy(src, in_ref.at[k], in_sem.at[k]) for k, src in enumerate(sources)]
    for load in loads:
        load.start()

    def fetch(k):
        loads[k].wait()
        return in_ref[k]

    def meet():
        around = jnp.where(is_root, n_leaf - 1, 1 + has_outer.astype(jnp.int32) + inner_is_other.astype(jnp.int32))
        pl.semaphore_wait(barrier, len(peers) + around)

    def parts(block):
        return n_mid if block in (CM, YM) else n_mid * n_top

    def height(block):
        if block in SYMMETRIC:
            return packed
        return r // parts(block) if block in PIECES else r

    def gram_copy(block, slot):
        place = slice(0, height(block))
        return pltpu.make_async_remote_copy(
            src_ref=bulk_ref.at[block, place], dst_ref=gram_in.at[slot, block, place],
            send_sem=gram_send.at[block], recv_sem=gram_recv.at[slot, block],
            device_id={"leaf": root}, device_id_type=MESH,
        )

    slot_here = lax.rem(root - leaf + n_leaf, n_leaf) - 1

    def store(ref, block, value, symmetric):
        if symmetric:
            main, diagonal = pack(value)
            ref[block, : r // 2] = main
            ref[block, r // 2 : packed] = diagonal
        else:
            ref[block] = value

    def piece_copy(block, number):
        a, b = peers[number]
        count, rows = parts(block), r // parts(block)
        there = beside(a, b)
        index = there["mid"] if count == n_mid else there["mid"] * n_top + there["top"]
        return pltpu.make_async_remote_copy(
            src_ref=raw_ref.at[PIECES.index(block), pl.ds(pl.multiple_of(index * rows, PANEL), rows)],
            dst_ref=piece_in.at[number, PIECES.index(block), slice(0, rows)],
            send_sem=piece_send.at[number, PIECES.index(block)], recv_sem=piece_recv.at[number, PIECES.index(block)],
            device_id=there, device_id_type=MESH,
        )

    def sharers(block):
        return [k for k, (a, b) in enumerate(peers) if b == 0 or parts(block) != n_mid]

    def own_place(block):
        rows = r // parts(block)
        index = mid if parts(block) == n_mid else mid * n_top + top
        return pl.ds(pl.multiple_of(index * rows, PANEL), rows)

    def share(block, value):
        raw_ref[PIECES.index(block)] = value
        for number in sharers(block):
            piece_copy(block, number).start()

    def join(block):
        k = PIECES.index(block)
        total = raw_ref[k, own_place(block)]
        for number in sharers(block):
            piece_copy(block, number).wait_recv()
            total = total + piece_in[number, k, : r // parts(block)]
        bulk_ref[block, : r // parts(block)] = total

    def give(block, value):
        store(bulk_ref, block, value, block in SYMMETRIC)

        if block not in LATER:
            @pl.when(is_other)
            def _():
                gram_copy(block, slot_here).start()

    prec, fine = fetch(0), fetch(1)
    solved_f = dot(prec, fine)
    s_ref[0] = solved_f
    gram_ff = dot(fine.T, solved_f)
    meet()
    give(FF, gram_ff)
    middle = fetch(2)
    mid_t = middle.T
    give(MF, dot(mid_t, solved_f))
    solved_m = dot(prec, middle)
    s_ref[1] = solved_m
    give(MM, dot(mid_t, solved_m))
    coarse = fetch(3)
    coarse_t = coarse.T
    give(CF, dot(coarse_t, solved_f))
    share(CM, dot(coarse_t, solved_m))
    solved_c = dot(prec, coarse)
    s_ref[2] = solved_c
    share(CC, dot(coarse_t, solved_c))
    obs = fetch(4)
    obs_t = obs.T
    share(YM, dot(obs_t, solved_m))
    share(YC, dot(obs_t, solved_c))
    give(YF, dot(obs_t, solved_f))
    s_ref[3] = dot(prec, obs)
    for k in range(5, 8):
        loads[k].wait()

    def gathered(block):
        place = slice(0, height(block))
        if block in PIECES:
            join(block)
        total = bulk_ref[block, place]
        for slot in range(n_leaf - 1):
            gram_copy(block, slot).wait_recv()
            total = total + gram_in[slot, block, place]
        return total

    def whole(value):
        return unpack(value[: r // 2], value[r // 2 :])

    def down_copy(block, slot, target):
        return pltpu.make_async_remote_copy(
            src_ref=down_ref.at[block], dst_ref=down_ref.at[block],
            send_sem=down_send.at[block, slot], recv_sem=down_recv.at[block],
            device_id={"leaf": target}, device_id_type=MESH,
        )

    def send_down(block, value):
        down_ref[block] = value
        for slot, exists in enumerate((root > 0, root < n_leaf - 1)):
            def go():
                down_copy(block, slot, root + 2 * slot - 1).start()

            if n_leaf > 2:
                go()
            else:
                pl.when(exists)(go)

    def pass_on(block):
        down_copy(block, 0, outer).wait_recv()

        @pl.when(has_outer)
        def _():
            down_copy(block, 0, outer).start()

    def cross_place(block):
        return slice(0, packed if block in (0, 3) else r)

    def cross_copy(block, step):
        return pltpu.make_async_remote_copy(
            src_ref=cross_ref.at[block, cross_place(block)], dst_ref=cross_in.at[step - 1, block, cross_place(block)],
            send_sem=cross_send.at[block, step - 1], recv_sem=cross_recv.at[block, step - 1],
            device_id={"mid": lax.rem(mid + step, n_mid)}, device_id_type=MESH,
        )

    def cross_start(block):
        for step in range(1, n_mid):
            cross_copy(block, step).start()

    def crossed(block):
        total = cross_ref[block, cross_place(block)]
        for step in range(1, n_mid):
            cross_copy(block, step).wait_recv()
            total = total + cross_in[step - 1, block, cross_place(block)]
        return total

    def corrected(raw, left_hand, right_rows):
        total_ref[...] = dot_nt(left_hand, right_rows)
        piece = gathered(raw)
        total_ref[own_place(raw)] = total_ref[own_place(raw)] + piece
        return total_ref[...]

    def last_place(block):
        return slice(0, r if block else packed)

    def last_copy(block, step):
        return pltpu.make_async_remote_copy(
            src_ref=last_ref.at[top, block, last_place(block)], dst_ref=last_ref.at[top, block, last_place(block)],
            send_sem=last_send.at[block, step - 1], recv_sem=last_recv.at[block, top],
            device_id=leaf_at(step), device_id_type=MESH,
        )

    def swap_copy(block, source, step):
        return pltpu.make_async_remote_copy(
            src_ref=last_ref.at[source, block, last_place(block)], dst_ref=last_ref.at[source, block, last_place(block)],
            send_sem=swap_send.at[block, step - 1], recv_sem=last_recv.at[block, source],
            device_id={"top": lax.rem(top + step, n_top)}, device_id_type=MESH,
        )

    def swap(block):
        for step in range(1, n_top):
            swap_copy(block, top, step).start()

    def send_last(block):
        for step in leaf_steps:
            last_copy(block, step).start()
        swap(block)

    def after_fine():
        s_ref[1] = s_ref[1] + dot_nt(s_ref[0], down_ref[0])
        s_ref[2] = s_ref[2] + dot_nt(s_ref[0], down_ref[1])

    @pl.when(is_root)
    def _():
        inverse = negated_inverse(a_ref, in_ref[5] + whole(gathered(FF)))
        mf = gathered(MF)
        n_m = dot(mf, inverse)
        store(cross_ref, 0, whole(gathered(MM)) + dot_nt(n_m, mf), True)
        cross_start(0)
        cf = gathered(CF)
        n_c = dot(cf, inverse)
        cross_ref[1] = corrected(CM, n_c, mf)
        cross_start(1)
        store(cross_ref, 3, corrected(CC, n_c, cf), True)
        cross_start(3)
        send_down(0, n_m)
        send_down(1, n_c)
        after_fine()
        n_y = dot(gathered(YF), inverse)
        cross_ref[2] = corrected(YM, n_y, mf)
        cross_start(2)
        cross_ref[4] = corrected(YC, n_y, cf)
        cross_start(4)
        send_down(2, n_y)

        inverse = negated_inverse(a_ref, in_ref[6] + whole(crossed(0)))
        cm = crossed(1)
        q_c = dot(cm, inverse)
        store(last_ref.at[top], 0, whole(crossed(3)) + dot_nt(q_c, cm), True)
        send_last(0)
        q_y = dot(crossed(2), inverse)
        last_ref[top, 1] = crossed(4) + dot_nt(q_y, cm)
        send_last(1)
        send_down(3, q_c)
        send_down(4, q_y)

    @pl.when(is_other)
    def _():
        for block in LATER:
            if block in PIECES:
                join(block)
            gram_copy(block, slot_here).start()
        pass_on(0)
        pass_on(1)
        pass_on(2)
        after_fine()
        last_copy(0, 1).wait_recv()
        swap(0)

    def others_arrived(block):
        for step in range(1, n_top):
            swap_copy(block, lax.rem(top + step, n_top), step).wait_recv()

    others_arrived(0)
    coarse_sum = last_ref[0, 0, :packed]
    for t in range(1, n_top):
        coarse_sum = coarse_sum + last_ref[t, 0, :packed]

    def middle_of_inverse():
        @pl.when(is_other)
        def _():
            last_copy(1, 1).wait_recv()
            swap(1)
            pass_on(3)

    inverse = negated_inverse(a_ref, in_ref[7] + whole(coarse_sum), middle_of_inverse)

    @pl.when(is_other)
    def _():
        pass_on(4)

    after_m = s_ref[1]
    after_c = s_ref[2] + dot_nt(after_m, down_ref[3])
    after_y = s_ref[3] + dot_nt(s_ref[0], down_ref[2]) + dot_nt(after_m, down_ref[4])
    others_arrived(1)
    right = last_ref[0, 1]
    for t in range(1, n_top):
        right = right + last_ref[t, 1]
    out_ref[...] = after_y + dot_nt(after_c, dot(right, inverse))

    for block in PIECES:
        for number in sharers(block):
            piece_copy(block, number).wait_send()
    for block in range(2):
        for step in range(1, n_top):
            swap_copy(block, top, step).wait_send()

    @pl.when(is_root)
    def _():
        for block in range(5):
            for step in range(1, n_mid):
                cross_copy(block, step).wait_send()
            for slot, exists in enumerate((root > 0, root < n_leaf - 1)):
                def done():
                    down_copy(block, slot, root + 2 * slot - 1).wait_send()

                if n_leaf > 2:
                    done()
                else:
                    pl.when(exists)(done)
        for block in range(2):
            for step in leaf_steps:
                last_copy(block, step).wait_send()

    @pl.when(is_other)
    def _():
        for block in range(9):
            gram_copy(block, slot_here).wait_send()

    @pl.when(has_outer)
    def _():
        for block in range(5):
            down_copy(block, 0, outer).wait_send()


def local(n_leaf, n_mid, n_top, *operands):
    blocks = [x.reshape(x.shape[-2:]) for x in operands]
    r = blocks[1].shape[1]
    f32 = jnp.float32
    dma = pltpu.SemaphoreType.DMA
    beside = max(n_mid * n_top - 1, 1)
    answer = pl.pallas_call(
        functools.partial(kernel, n_leaf, n_mid, n_top),
        out_shape=jax.ShapeDtypeStruct(blocks[-1].shape, f32),
        in_specs=[pl.BlockSpec(memory_space=pl.ANY)] * len(blocks),
        out_specs=pl.BlockSpec(memory_space=pltpu.VMEM),
        scratch_shapes=[
            pltpu.VMEM((8, r, r), f32),
            pltpu.VMEM((r + 2 * PANEL, r), f32),
            pltpu.VMEM((4, r, r), f32),
            pltpu.VMEM((4, r, r), f32),
            pltpu.VMEM((9, r, r), f32),
            pltpu.VMEM((beside, 4, r // n_mid, r), f32),
            pltpu.VMEM((n_leaf - 1, 9, r, r), f32),
            pltpu.VMEM((r, r), f32),
            pltpu.VMEM((5, r, r), f32),
            pltpu.VMEM((5, r, r), f32),
            pltpu.VMEM((n_mid - 1, 5, r, r), f32),
            pltpu.VMEM((n_top, 2, r, r), f32),
            dma((8,)),
            dma((beside, 4)), dma((beside, 4)),
            dma((9,)), dma((n_leaf - 1, 9)),
            dma((5, 2)), dma((5,)),
            dma((5, n_mid - 1)), dma((5, n_mid - 1)),
            dma((2, n_leaf - 1)), dma((2, n_top)), dma((2, n_top - 1)),
        ],
        compiler_params=pltpu.CompilerParams(collective_id=0, has_side_effects=True),
    )(*blocks)
    return answer[None, None, None]


def solution(mesh):
    spread = P(("parts", "leaf"), "mid", "top", None, None)
    sizes = (mesh.shape["leaf"], mesh.shape["mid"], mesh.shape["top"])
    return jax.shard_map(
        functools.partial(local, *sizes),
        mesh=mesh,
        in_specs=(spread, spread, spread, spread, P(), P(), P(), spread),
        out_specs=spread,
        check_vma=False,
    )
```

```python
import functools

import jax
import jax.numpy as jnp
from jax import lax
from jax.experimental import pallas as pl
from jax.experimental.pallas import tpu as pltpu
from jax.sharding import PartitionSpec as P

MESH = pl.DeviceIdType.MESH
PANEL = 8
VMEM_ROOM = 56_558_000


def dot(left_hand, right_side):
    return jnp.dot(
        left_hand, right_side, precision=lax.Precision.HIGHEST, preferred_element_type=jnp.float32
    )


def split3(x):
    high = x.astype(jnp.bfloat16).astype(jnp.float32)
    rest = x - high
    mid = rest.astype(jnp.bfloat16).astype(jnp.float32)
    low = (rest - mid).astype(jnp.bfloat16).astype(jnp.float32)
    return high, mid, low


def spread_panel(panel):
    p1, p2, p3 = split3(panel)
    return jnp.concatenate([p1, p1, p2, p2, p1, p3], axis=0).T.astype(jnp.bfloat16)


def rank_update(spread, scaled):
    r1, r2, r3 = split3(scaled)
    right_side = jnp.concatenate([r1, r2, r1, r2, r3, r1], axis=0).astype(jnp.bfloat16)
    return jnp.dot(spread, right_side, preferred_element_type=jnp.float32)


def negated_inverse(a_ref, matrix, between=None):
    size = matrix.shape[0]
    zero = jnp.zeros((PANEL, size), jnp.float32)
    a_ref[pl.ds(0, PANEL), :] = zero
    a_ref[pl.ds(PANEL, size), :] = matrix
    a_ref[pl.ds(PANEL + size, PANEL), :] = zero
    lane = lax.broadcasted_iota(jnp.int32, (PANEL, size), 1)
    sub = lax.broadcasted_iota(jnp.int32, (PANEL, size), 0)
    lane_full = lax.broadcasted_iota(jnp.int32, (size, size), 1)

    def lanes(block, index):
        picked = jnp.where(lane == index, block, 0.0)
        return jnp.broadcast_to(jnp.sum(picked, axis=1, keepdims=True), block.shape)

    def row_of(block, i):
        return jnp.broadcast_to(block[i : i + 1], block.shape)

    def apply(k, spread, scaled):
        inside = (lane_full >= k * PANEL) & (lane_full < (k + 1) * PANEL)
        current = a_ref[pl.ds(PANEL, size), :]
        a_ref[pl.ds(PANEL, size), :] = jnp.where(inside, 0.0, current) - rank_update(spread, scaled)
        a_ref[pl.ds(pl.multiple_of((k + 1) * PANEL, PANEL), PANEL), :] = scaled

    def body(k, carry):
        spread_before, scaled_before, panel = carry
        apply(k - 1, spread_before, scaled_before)
        inside = (lane >= k * PANEL) & (lane < (k + 1) * PANEL)
        cols = [lanes(panel, k * PANEL + j) for j in range(PANEL)]
        ahead = (k + 1) * PANEL + sub
        below = [lanes(row_of(panel, j), ahead) for j in range(PANEL)]
        spread = spread_panel(panel)
        following = a_ref[pl.ds(pl.multiple_of((k + 2) * PANEL, PANEL), PANEL), :]
        x = jnp.where(inside, jnp.where(lane - k * PANEL == sub, 1.0, 0.0), panel)
        gone = jnp.zeros_like(x)
        scale = gone
        for i in range(PANEL):
            pivot = 1.0 / row_of(cols[i], i)
            here = sub == i
            factor = jnp.where(here, 0.0, cols[i])
            row = row_of(x, i)
            across, down = factor * pivot, below[i] * pivot
            for j in range(i + 1, PANEL):
                entry = row_of(cols[j], i)
                if j == i + 1:
                    cols[j] = cols[j] - (factor * entry) * pivot
                else:
                    cols[j] = cols[j] - across * entry
                below[j] = below[j] - down * entry
            x = x - across * row
            gone = gone + down * row
            scale = jnp.where(here, pivot, scale)
        x = x * scale
        return spread, jnp.where(inside, -x, x), jnp.where(inside, gone, following - gone)

    steps = size // PANEL
    carry = (spread_panel(zero), zero, matrix[:PANEL])
    if between is None:
        spread, scaled, _ = lax.fori_loop(0, steps, body, carry)
    else:
        carry = lax.fori_loop(0, steps // 2, body, carry)
        between()
        spread, scaled, _ = lax.fori_loop(steps // 2, steps, body, carry)
    apply(steps - 1, spread, scaled)
    return a_ref[pl.ds(PANEL, size), :]


def dot_nt(left_hand, right_rows):
    return lax.dot_general(
        left_hand, right_rows, (((1,), (1,)), ((), ())),
        precision=lax.Precision.HIGHEST, preferred_element_type=jnp.float32,
    )


def pack(matrix):
    half, size = matrix.shape[0] // 2, matrix.shape[1]
    lane = lax.broadcasted_iota(jnp.int32, (PANEL, size), 1)
    blocks = [matrix[:PANEL]]
    for start in range(PANEL, half + 1, PANEL):
        moved = pltpu.roll(matrix[size - start : size - start + PANEL], start, 1)
        blocks.append(moved if start == half else jnp.where(lane < start, moved, matrix[start : start + PANEL]))
    return jnp.concatenate(blocks, axis=0)


def unpack(packed):
    half, size = packed.shape[0] - PANEL, packed.shape[1]
    bottom = [pltpu.roll(packed[start : start + PANEL], size - start, 1) for start in range(half, 0, -PANEL)]
    return jnp.concatenate([packed[:half], *bottom], axis=0)


FF, MF, MM, CF, CM, YF, YM, CC, YC = range(9)
SYMMETRIC = (FF, MM)
LATER = (CM, CC, YF, YM, YC)
PIECES = (CM, YM, CC, YC)
SEEN = (YF, YM, YC)


def kernel(
    n_leaf, n_mid, n_top,
    prec_hbm, fine_hbm, mid_hbm, coarse_hbm, core_fine_hbm, core_mid_hbm, core_coarse_hbm, obs_hbm,
    out_ref,
    in_ref, a_ref, s_ref, raw_ref, bulk_ref, piece_in, gram_in, total_ref, kept_ref, down_ref, cross_ref, cross_in, last_ref, seen_in, answer_ref,
    in_sem, piece_send, piece_recv, gram_send, gram_recv, down_send, down_recv, spread_send,
    cross_send, cross_recv, last_send, last_recv, swap_send, seen_recv, help_send, help_recv, answer_send,
):
    r = bulk_ref.shape[1]
    packed = r // 2 + PANEL
    leaf, mid, top = lax.axis_index("leaf"), lax.axis_index("mid"), lax.axis_index("top")
    low, high = (n_leaf - 1) // 2, n_leaf // 2

    def root_of(index):
        return low + lax.rem(index, 2) * (high - low)

    root = root_of(top)
    after_top, before_top = lax.rem(top + 1, n_top), lax.rem(top + n_top - 1, n_top)
    is_helper = leaf == root_of(before_top)
    is_root = leaf == root
    is_other = leaf != root
    side = (leaf > root).astype(jnp.int32)
    inner, outer = leaf + 1 - 2 * side, leaf - 1 + 2 * side
    has_outer = is_other & (outer >= 0) & (outer < n_leaf)
    inner_is_other = is_other & (inner != root)
    barrier = pltpu.get_barrier_semaphore()

    def greet(device):
        pl.semaphore_signal(barrier, inc=1, device_id=device, device_id_type=MESH)

    leaf_steps = sorted(range(1, n_leaf), key=lambda step: (abs(2 * step - n_leaf), step))
    peers = [(a, b) for a in range(n_mid) for b in range(n_top) if (a, b) != (0, 0)]

    def beside(a, b):
        return {"mid": lax.rem(mid + a, n_mid), "top": lax.rem(top + b, n_top)}

    def leaf_at(step):
        return {"leaf": lax.rem(leaf + step, n_leaf)}

    for a, b in peers:
        greet(beside(a, b))

    @pl.when(is_root)
    def _():
        for step in leaf_steps:
            greet(leaf_at(step))

    @pl.when(is_other)
    def _():
        greet({"leaf": root})

        greet({"leaf": root, "top": after_top})

    @pl.when(is_helper)
    def _():
        for step in leaf_steps:
            greet({**leaf_at(step), "top": before_top})

    @pl.when(has_outer)
    def _():
        greet({"leaf": outer})

    @pl.when(inner_is_other)
    def _():
        greet({"leaf": inner})

    sources = [prec_hbm, fine_hbm, mid_hbm, coarse_hbm, obs_hbm, core_fine_hbm, core_mid_hbm, core_coarse_hbm]
    loads = [pltpu.make_async_copy(src, in_ref.at[k], in_sem.at[k]) for k, src in enumerate(sources)]
    for load in loads:
        load.start()

    def fetch(k):
        loads[k].wait()
        return in_ref[k]

    def meet():
        around = jnp.where(is_root, n_leaf - 1, 2 + has_outer.astype(jnp.int32) + inner_is_other.astype(jnp.int32))
        helped = jnp.where(is_helper, n_leaf - 1, 0)
        pl.semaphore_wait(barrier, len(peers) + around + helped)

    def parts(block):
        return n_mid if block in (CM, YM) else n_mid * n_top

    def height(block):
        if block in SYMMETRIC:
            return packed
        return r // parts(block) if block in PIECES else r

    def gram_copy(block, slot):
        place = slice(0, height(block))
        return pltpu.make_async_remote_copy(
            src_ref=bulk_ref.at[block, place], dst_ref=gram_in.at[slot, block, place],
            send_sem=gram_send.at[block], recv_sem=gram_recv.at[slot, block],
            device_id={"leaf": root}, device_id_type=MESH,
        )

    slot_here = lax.rem(root - leaf + n_leaf, n_leaf) - 1

    def seen_copy(block, slot):
        place = slice(0, height(block))
        return pltpu.make_async_remote_copy(
            src_ref=bulk_ref.at[block, place], dst_ref=seen_in.at[slot, SEEN.index(block), place],
            send_sem=gram_send.at[block], recv_sem=seen_recv.at[slot, SEEN.index(block)],
            device_id={"leaf": root, "top": after_top}, device_id_type=MESH,
        )

    def store(ref, block, value, symmetric):
        if symmetric:
            ref[block, :packed] = pack(value)
        else:
            ref[block] = value

    def piece_copy(block, number):
        a, b = peers[number]
        count, rows = parts(block), r // parts(block)
        there = beside(a, b)
        index = there["mid"] if count == n_mid else there["mid"] * n_top + there["top"]
        return pltpu.make_async_remote_copy(
            src_ref=raw_ref.at[PIECES.index(block), pl.ds(pl.multiple_of(index * rows, PANEL), rows)],
            dst_ref=piece_in.at[number, PIECES.index(block), slice(0, rows)],
            send_sem=piece_send.at[number, PIECES.index(block)], recv_sem=piece_recv.at[number, PIECES.index(block)],
            device_id=there, device_id_type=MESH,
        )

    def sharers(block):
        return [k for k, (a, b) in enumerate(peers) if b == 0 or parts(block) != n_mid]

    def own_place(block, group):
        rows = r // parts(block)
        index = mid if parts(block) == n_mid else mid * n_top + group
        return pl.ds(pl.multiple_of(index * rows, PANEL), rows)

    def share(block, value):
        raw_ref[PIECES.index(block)] = value
        for number in sharers(block):
            piece_copy(block, number).start()

    def join(block):
        k = PIECES.index(block)
        total = raw_ref[k, own_place(block, top)]
        for number in sharers(block):
            piece_copy(block, number).wait_recv()
            total = total + piece_in[number, k, : r // parts(block)]
        bulk_ref[block, : r // parts(block)] = total

    def give(block, value):
        store(bulk_ref, block, value, block in SYMMETRIC)

        if block not in LATER:
            @pl.when(is_other)
            def _():
                gram_copy(block, slot_here).start()

    prec, fine = fetch(0), fetch(1)
    solved_f = dot(prec, fine)
    s_ref[0] = solved_f
    gram_ff = dot(fine.T, solved_f)
    meet()
    give(FF, gram_ff)
    middle = fetch(2)
    mid_t = middle.T
    give(MF, dot(mid_t, solved_f))
    solved_m = dot(prec, middle)
    s_ref[1] = solved_m
    give(MM, dot(mid_t, solved_m))
    coarse = fetch(3)
    coarse_t = coarse.T
    give(CF, dot(coarse_t, solved_f))
    share(CM, dot(coarse_t, solved_m))
    solved_c = dot(prec, coarse)
    s_ref[2] = solved_c
    share(CC, dot(coarse_t, solved_c))
    obs = fetch(4)
    obs_t = obs.T
    share(YM, dot(obs_t, solved_m))
    share(YC, dot(obs_t, solved_c))
    give(YF, dot(obs_t, solved_f))
    s_ref[3] = dot(prec, obs)
    for k in range(5, 8):
        loads[k].wait()

    def gathered(block):
        place = slice(0, height(block))
        if block in PIECES:
            join(block)
        total = bulk_ref[block, place]
        for slot in range(n_leaf - 1):
            gram_copy(block, slot).wait_recv()
            total = total + gram_in[slot, block, place]
        return total

    def down_copy(block, slot, target):
        return pltpu.make_async_remote_copy(
            src_ref=down_ref.at[block], dst_ref=down_ref.at[block],
            send_sem=down_send.at[block, slot], recv_sem=down_recv.at[block],
            device_id={"leaf": target}, device_id_type=MESH,
        )

    def send_down(block, value):
        down_ref[block] = value
        for slot, exists in enumerate((root > 0, root < n_leaf - 1)):
            def go():
                down_copy(block, slot, root + 2 * slot - 1).start()

            if n_leaf > 2:
                go()
            else:
                pl.when(exists)(go)

    def spread_copy(block, step):
        return pltpu.make_async_remote_copy(
            src_ref=down_ref.at[block], dst_ref=down_ref.at[block],
            send_sem=spread_send.at[block - 3, step - 1], recv_sem=down_recv.at[block],
            device_id=leaf_at(step), device_id_type=MESH,
        )

    def send_all(block, value):
        down_ref[block] = value
        for step in leaf_steps:
            spread_copy(block, step).start()

    def pass_on(block):
        down_copy(block, 0, outer).wait_recv()

        @pl.when(has_outer)
        def _():
            down_copy(block, 0, outer).start()

    def seen(block):
        place = slice(0, height(block))
        for slot in range(n_leaf):
            seen_copy(block, slot).wait_recv()
        total = seen_in[0, SEEN.index(block), place]
        for slot in range(1, n_leaf):
            total = total + seen_in[slot, SEEN.index(block), place]
        return total

    def help_copy(number):
        return pltpu.make_async_remote_copy(
            src_ref=kept_ref.at[number], dst_ref=kept_ref.at[number],
            send_sem=help_send.at[number], recv_sem=help_recv.at[number],
            device_id={"top": after_top}, device_id_type=MESH,
        )

    def keep(number, value):
        kept_ref[number] = value
        help_copy(number).start()

    def answer_copy(number, step):
        target, arrival = (
            (down_ref.at[2], down_recv.at[2]),
            (last_ref.at[before_top, 1], last_recv.at[1, before_top]),
            (down_ref.at[4], down_recv.at[4]),
        )[number]
        return pltpu.make_async_remote_copy(
            src_ref=answer_ref.at[number], dst_ref=target,
            send_sem=answer_send.at[number, step], recv_sem=arrival,
            device_id={**leaf_at(step), "top": before_top}, device_id_type=MESH,
        )

    def send_answer(number, value):
        answer_ref[number] = value
        for step in [*leaf_steps, 0]:
            answer_copy(number, step).start()

    def cross_place(block):
        return slice(0, packed if block in (0, 3) else r)

    def cross_copy(block, step):
        return pltpu.make_async_remote_copy(
            src_ref=cross_ref.at[block, cross_place(block)], dst_ref=cross_in.at[step - 1, block, cross_place(block)],
            send_sem=cross_send.at[block, step - 1], recv_sem=cross_recv.at[block, step - 1],
            device_id={"mid": lax.rem(mid + step, n_mid)}, device_id_type=MESH,
        )

    def cross_start(block):
        for step in range(1, n_mid):
            cross_copy(block, step).start()

    def crossed(block):
        total = cross_ref[block, cross_place(block)]
        for step in range(1, n_mid):
            cross_copy(block, step).wait_recv()
            total = total + cross_in[step - 1, block, cross_place(block)]
        return total

    def corrected(raw, value):
        total_ref[...] = value
        piece, group = (seen(raw), before_top) if raw in SEEN else (gathered(raw), top)
        total_ref[own_place(raw, group)] = total_ref[own_place(raw, group)] + piece
        return total_ref[...]

    def last_place(block):
        return slice(0, r if block else packed)

    def last_copy(block, step):
        return pltpu.make_async_remote_copy(
            src_ref=last_ref.at[top, block, last_place(block)], dst_ref=last_ref.at[top, block, last_place(block)],
            send_sem=last_send.at[block, step - 1], recv_sem=last_recv.at[block, top],
            device_id=leaf_at(step), device_id_type=MESH,
        )

    def swap_copy(block, source, step):
        return pltpu.make_async_remote_copy(
            src_ref=last_ref.at[source, block, last_place(block)], dst_ref=last_ref.at[source, block, last_place(block)],
            send_sem=swap_send.at[block, step - 1], recv_sem=last_recv.at[block, source],
            device_id={"top": lax.rem(top + step, n_top)}, device_id_type=MESH,
        )

    def swap(block):
        for step in range(1, n_top):
            swap_copy(block, top, step).start()

    def send_last(block):
        for step in leaf_steps:
            last_copy(block, step).start()
        swap(block)

    def after_fine():
        s_ref[1] = s_ref[1] + dot_nt(s_ref[0], down_ref[0])
        s_ref[2] = s_ref[2] + dot_nt(s_ref[0], down_ref[1])
        s_ref[3] = s_ref[3] + dot_nt(s_ref[0], down_ref[2])

    @pl.when(is_root)
    def _():
        inverse = negated_inverse(a_ref, in_ref[5] + unpack(gathered(FF)))
        mf = gathered(MF)
        n_m = dot(mf, inverse)
        store(cross_ref, 0, unpack(gathered(MM)) + dot_nt(n_m, mf), True)
        cross_start(0)
        keep(0, inverse)
        keep(1, mf)
        cf = gathered(CF)
        n_c = dot(cf, inverse)
        keep(2, cf)
        lost = dot_nt(n_c, kept_ref[1:3].reshape(2 * r, r))
        cross_ref[1] = corrected(CM, lost[:, :r])
        cross_start(1)
        store(cross_ref, 3, corrected(CC, lost[:, r:]), True)
        cross_start(3)
        for block in SEEN:
            if block in PIECES:
                join(block)
            seen_copy(block, 0).start()
        send_down(0, n_m)
        send_down(1, n_c)

        inverse = negated_inverse(a_ref, in_ref[6] + unpack(crossed(0)))
        cm = crossed(1)
        q_c = dot(cm, inverse)
        store(last_ref.at[top], 0, unpack(crossed(3)) + dot_nt(q_c, cm), True)
        send_last(0)
        keep(3, inverse)
        keep(4, cm)
        send_all(3, q_c)
        down_copy(2, 0, outer).wait_recv()
        after_fine()

    @pl.when(is_other)
    def _():
        for block in LATER:
            if block in PIECES:
                join(block)
            if block in SEEN:
                seen_copy(block, slot_here + 1).start()
            else:
                gram_copy(block, slot_here).start()

    @pl.when(is_helper)
    def _():
        for number in range(2):
            help_copy(number).wait_recv()
        n_y = dot(seen(YF), kept_ref[0])
        help_copy(2).wait_recv()
        lost = dot_nt(n_y, kept_ref[1:3].reshape(2 * r, r))
        cross_ref[2] = corrected(YM, lost[:, :r])
        cross_start(2)
        cross_ref[4] = corrected(YC, lost[:, r:])
        cross_start(4)
        send_answer(0, n_y)

    @pl.when(is_other)
    def _():
        pass_on(0)
        pass_on(1)

    @pl.when(is_helper)
    def _():
        for number in range(3, 5):
            help_copy(number).wait_recv()
        q_y = dot(crossed(2), kept_ref[3])
        send_answer(1, crossed(4) + dot_nt(q_y, kept_ref[4]))
        send_answer(2, q_y)

    @pl.when(is_other)
    def _():
        down_copy(2, 0, outer).wait_recv()
        after_fine()
        last_copy(0, 1).wait_recv()
        swap(0)

    def others_arrived(block):
        for step in range(1, n_top):
            swap_copy(block, lax.rem(top + step, n_top), step).wait_recv()

    others_arrived(0)
    coarse_sum = last_ref[0, 0, :packed]
    for t in range(1, n_top):
        coarse_sum = coarse_sum + last_ref[t, 0, :packed]

    def middle_of_inverse():
        last_copy(1, 1).wait_recv()
        swap(1)

    inverse = negated_inverse(a_ref, in_ref[7] + unpack(coarse_sum), middle_of_inverse)

    @pl.when(is_other)
    def _():
        spread_copy(3, 1).wait_recv()

    spread_copy(4, 1).wait_recv()
    others_arrived(1)
    right = last_ref[0, 1]
    for t in range(1, n_top):
        right = right + last_ref[t, 1]
    after = dot_nt(s_ref[1], down_ref[3:5].reshape(2 * r, r))
    out_ref[...] = s_ref[3] + after[:, r:] + dot_nt(s_ref[2] + after[:, :r], dot(right, inverse))

    for block in PIECES:
        for number in sharers(block):
            piece_copy(block, number).wait_send()
    for block in range(2):
        for step in range(1, n_top):
            swap_copy(block, top, step).wait_send()

    @pl.when(is_root)
    def _():
        for block in (0, 1, 3):
            for step in range(1, n_mid):
                cross_copy(block, step).wait_send()
        for step in leaf_steps:
            spread_copy(3, step).wait_send()
            last_copy(0, step).wait_send()
        for number in range(5):
            help_copy(number).wait_send()
        for block in SEEN:
            seen_copy(block, 0).wait_send()
        for block in range(2):
            for slot, exists in enumerate((root > 0, root < n_leaf - 1)):
                def done():
                    down_copy(block, slot, root + 2 * slot - 1).wait_send()

                if n_leaf > 2:
                    done()
                else:
                    pl.when(exists)(done)

    @pl.when(is_helper)
    def _():
        for block in (2, 4):
            for step in range(1, n_mid):
                cross_copy(block, step).wait_send()
        for number in range(3):
            for step in range(n_leaf):
                answer_copy(number, step).wait_send()

    @pl.when(is_other)
    def _():
        for block in range(9):
            gram_copy(block, slot_here).wait_send()

    @pl.when(has_outer)
    def _():
        for block in range(2):
            down_copy(block, 0, outer).wait_send()


def local(n_leaf, n_mid, n_top, *operands):
    blocks = [x.reshape(x.shape[-2:]) for x in operands]
    r = blocks[1].shape[1]
    f32 = jnp.float32
    dma = pltpu.SemaphoreType.DMA
    beside = max(n_mid * n_top - 1, 1)
    answer = pl.pallas_call(
        functools.partial(kernel, n_leaf, n_mid, n_top),
        out_shape=jax.ShapeDtypeStruct(blocks[-1].shape, f32),
        in_specs=[pl.BlockSpec(memory_space=pl.ANY)] * len(blocks),
        out_specs=pl.BlockSpec(memory_space=pltpu.VMEM),
        scratch_shapes=[
            pltpu.VMEM((8, r, r), f32),
            pltpu.VMEM((r + 2 * PANEL, r), f32),
            pltpu.VMEM((4, r, r), f32),
            pltpu.VMEM((4, r, r), f32),
            pltpu.VMEM((9, r, r), f32),
            pltpu.VMEM((beside, 4, r // n_mid, r), f32),
            pltpu.VMEM((n_leaf - 1, 9, r, r), f32),
            pltpu.VMEM((r, r), f32),
            pltpu.VMEM((5, r, r), f32),
            pltpu.VMEM((5, r, r), f32),
            pltpu.VMEM((5, r, r), f32),
            pltpu.VMEM((n_mid - 1, 5, r, r), f32),
            pltpu.VMEM((n_top, 2, r, r), f32),
            pltpu.VMEM((n_leaf, 3, r, r), f32),
            pltpu.VMEM((3, r, r), f32),
            dma((8,)),
            dma((beside, 4)), dma((beside, 4)),
            dma((9,)), dma((n_leaf - 1, 9)),
            dma((3, 2)), dma((5,)), dma((2, n_leaf - 1)),
            dma((5, n_mid - 1)), dma((5, n_mid - 1)),
            dma((2, n_leaf - 1)), dma((2, n_top)), dma((2, n_top - 1)),
            dma((n_leaf, 3)), dma((5,)), dma((5,)), dma((3, n_leaf)),
        ],
        compiler_params=pltpu.CompilerParams(
            collective_id=0, has_side_effects=True, vmem_limit_bytes=VMEM_ROOM - 3 * r * blocks[-1].shape[1] * 2,
        ),
    )(*blocks)
    return answer[None, None, None]


def solution(mesh):
    spread = P(("parts", "leaf"), "mid", "top", None, None)
    sizes = (mesh.shape["leaf"], mesh.shape["mid"], mesh.shape["top"])
    return jax.shard_map(
        functools.partial(local, *sizes),
        mesh=mesh,
        in_specs=(spread, spread, spread, spread, P(), P(), P(), spread),
        out_specs=spread,
        check_vma=False,
    )
```

```python
import functools

import jax
import jax.numpy as jnp
from jax import lax
from jax.experimental import pallas as pl
from jax.experimental.pallas import tpu as pltpu
from jax.sharding import PartitionSpec as P

MESH = pl.DeviceIdType.MESH
PANEL = 8
VMEM_ROOM = 56_558_000


def dot(left_hand, right_side):
    return jnp.dot(
        left_hand, right_side, precision=lax.Precision.HIGHEST, preferred_element_type=jnp.float32
    )


def split3(x):
    high = x.astype(jnp.bfloat16).astype(jnp.float32)
    rest = x - high
    mid = rest.astype(jnp.bfloat16).astype(jnp.float32)
    low = (rest - mid).astype(jnp.bfloat16).astype(jnp.float32)
    return high, mid, low


def spread_panel(panel):
    p1, p2, p3 = split3(panel)
    return jnp.concatenate([p1, p1, p2, p2, p1, p3], axis=0).T.astype(jnp.bfloat16)


def rank_update(spread, scaled):
    r1, r2, r3 = split3(scaled)
    right_side = jnp.concatenate([r1, r2, r1, r2, r3, r1], axis=0).astype(jnp.bfloat16)
    return jnp.dot(spread, right_side, preferred_element_type=jnp.float32)


def negated_inverse(a_ref, matrix, between=None):
    size = matrix.shape[0]
    zero = jnp.zeros((PANEL, size), jnp.float32)
    a_ref[pl.ds(0, PANEL), :] = zero
    a_ref[pl.ds(PANEL, size), :] = matrix
    a_ref[pl.ds(PANEL + size, PANEL), :] = zero
    lane = lax.broadcasted_iota(jnp.int32, (PANEL, size), 1)
    sub = lax.broadcasted_iota(jnp.int32, (PANEL, size), 0)
    lane_full = lax.broadcasted_iota(jnp.int32, (size, size), 1)

    def lanes(block, index):
        picked = jnp.where(lane == index, block, 0.0)
        return jnp.broadcast_to(jnp.sum(picked, axis=1, keepdims=True), block.shape)

    def row_of(block, i):
        return jnp.broadcast_to(block[i : i + 1], block.shape)

    def apply(k, spread, scaled):
        inside = (lane_full >= k * PANEL) & (lane_full < (k + 1) * PANEL)
        current = a_ref[pl.ds(PANEL, size), :]
        a_ref[pl.ds(PANEL, size), :] = jnp.where(inside, 0.0, current) - rank_update(spread, scaled)
        a_ref[pl.ds(pl.multiple_of((k + 1) * PANEL, PANEL), PANEL), :] = scaled

    def body(k, carry):
        spread_before, scaled_before, panel = carry
        apply(k - 1, spread_before, scaled_before)
        inside = (lane >= k * PANEL) & (lane < (k + 1) * PANEL)
        cols = [lanes(panel, k * PANEL + j) for j in range(PANEL)]
        ahead = (k + 1) * PANEL + sub
        below = [lanes(row_of(panel, j), ahead) for j in range(PANEL)]
        spread = spread_panel(panel)
        following = a_ref[pl.ds(pl.multiple_of((k + 2) * PANEL, PANEL), PANEL), :]
        x = jnp.where(inside, jnp.where(lane - k * PANEL == sub, 1.0, 0.0), panel)
        gone = jnp.zeros_like(x)
        scale = gone
        for i in range(PANEL):
            pivot = 1.0 / row_of(cols[i], i)
            here = sub == i
            factor = jnp.where(here, 0.0, cols[i])
            row = row_of(x, i)
            across, down = factor * pivot, below[i] * pivot
            for j in range(i + 1, PANEL):
                entry = row_of(cols[j], i)
                if j == i + 1:
                    cols[j] = cols[j] - (factor * entry) * pivot
                else:
                    cols[j] = cols[j] - across * entry
                below[j] = below[j] - down * entry
            x = x - across * row
            gone = gone + down * row
            scale = jnp.where(here, pivot, scale)
        x = x * scale
        return spread, jnp.where(inside, -x, x), jnp.where(inside, gone, following - gone)

    steps = size // PANEL
    carry = (spread_panel(zero), zero, matrix[:PANEL])
    if between is None:
        spread, scaled, _ = lax.fori_loop(0, steps, body, carry)
    else:
        carry = lax.fori_loop(0, steps // 2, body, carry)
        between()
        spread, scaled, _ = lax.fori_loop(steps // 2, steps, body, carry)
    apply(steps - 1, spread, scaled)
    return a_ref[pl.ds(PANEL, size), :]


def dot_nt(left_hand, right_rows):
    return lax.dot_general(
        left_hand, right_rows, (((1,), (1,)), ((), ())),
        precision=lax.Precision.HIGHEST, preferred_element_type=jnp.float32,
    )


def pack(matrix):
    half, size = matrix.shape[0] // 2, matrix.shape[1]
    lane = lax.broadcasted_iota(jnp.int32, (PANEL, size), 1)
    blocks = [matrix[:PANEL]]
    for start in range(PANEL, half + 1, PANEL):
        moved = pltpu.roll(matrix[size - start : size - start + PANEL], start, 1)
        blocks.append(moved if start == half else jnp.where(lane < start, moved, matrix[start : start + PANEL]))
    return jnp.concatenate(blocks, axis=0)


def unpack(packed):
    half, size = packed.shape[0] - PANEL, packed.shape[1]
    bottom = [pltpu.roll(packed[start : start + PANEL], size - start, 1) for start in range(half, 0, -PANEL)]
    return jnp.concatenate([packed[:half], *bottom], axis=0)


FF, MF, MM, CF, CM, YF, YM, CC, YC = range(9)
SYMMETRIC = (FF, MM)
LATER = (CM, CC, YF, YM, YC)
PIECES = (CM, YM, CC, YC)
SEEN = (YF, YM, YC)


def kernel(
    n_leaf, n_mid, n_top,
    prec_hbm, fine_hbm, mid_hbm, coarse_hbm, core_fine_hbm, core_mid_hbm, core_coarse_hbm, obs_hbm,
    out_ref,
    in_ref, a_ref, s_ref, raw_ref, bulk_ref, piece_in, gram_in, total_ref, kept_ref, down_ref, cross_ref, cross_in, last_ref, seen_in, answer_ref,
    in_sem, piece_send, piece_recv, gram_send, gram_recv, down_send, down_recv, spread_send,
    cross_send, cross_recv, last_send, last_recv, swap_send, seen_recv, help_send, help_recv, answer_send,
):
    r = bulk_ref.shape[1]
    packed = r // 2 + PANEL
    leaf, mid, top = lax.axis_index("leaf"), lax.axis_index("mid"), lax.axis_index("top")
    low, high = (n_leaf - 1) // 2, n_leaf // 2

    def root_of(index):
        return low + lax.rem(index, 2) * (high - low)

    root = root_of(top)
    after_top, before_top = lax.rem(top + 1, n_top), lax.rem(top + n_top - 1, n_top)
    is_helper = leaf == root_of(before_top)
    is_root = leaf == root
    is_other = leaf != root
    side = (leaf > root).astype(jnp.int32)
    inner, outer = leaf + 1 - 2 * side, leaf - 1 + 2 * side
    has_outer = is_other & (outer >= 0) & (outer < n_leaf)
    inner_is_other = is_other & (inner != root)
    barrier = pltpu.get_barrier_semaphore()

    def greet(device):
        pl.semaphore_signal(barrier, inc=1, device_id=device, device_id_type=MESH)

    leaf_steps = sorted(range(1, n_leaf), key=lambda step: (abs(2 * step - n_leaf), step))
    peers = [(a, b) for a in range(n_mid) for b in range(n_top) if (a, b) != (0, 0)]

    def beside(a, b):
        return {"mid": lax.rem(mid + a, n_mid), "top": lax.rem(top + b, n_top)}

    def leaf_at(step):
        return {"leaf": lax.rem(leaf + step, n_leaf)}

    for a, b in peers:
        greet(beside(a, b))

    @pl.when(is_root)
    def _():
        for step in leaf_steps:
            greet(leaf_at(step))

    @pl.when(is_other)
    def _():
        greet({"leaf": root})

        greet({"leaf": root, "top": after_top})

    @pl.when(is_helper)
    def _():
        for step in leaf_steps:
            greet({**leaf_at(step), "top": before_top})

    @pl.when(has_outer)
    def _():
        greet({"leaf": outer})

    @pl.when(inner_is_other)
    def _():
        greet({"leaf": inner})

    sources = [prec_hbm, fine_hbm, mid_hbm, coarse_hbm, obs_hbm, core_fine_hbm, core_mid_hbm, core_coarse_hbm]
    loads = [pltpu.make_async_copy(src, in_ref.at[k], in_sem.at[k]) for k, src in enumerate(sources)]
    for load in loads:
        load.start()

    def fetch(k):
        loads[k].wait()
        return in_ref[k]

    def meet():
        around = jnp.where(is_root, n_leaf - 1, 2 + has_outer.astype(jnp.int32) + inner_is_other.astype(jnp.int32))
        helped = jnp.where(is_helper, n_leaf - 1, 0)
        pl.semaphore_wait(barrier, len(peers) + around + helped)

    def parts(block):
        return n_mid if block in (CM, YM) else n_mid * n_top

    def height(block):
        if block in SYMMETRIC:
            return packed
        return r // parts(block) if block in PIECES else r

    def gram_copy(block, slot):
        place = slice(0, height(block))
        return pltpu.make_async_remote_copy(
            src_ref=bulk_ref.at[block, place], dst_ref=gram_in.at[slot, block, place],
            send_sem=gram_send.at[block], recv_sem=gram_recv.at[slot, block],
            device_id={"leaf": root}, device_id_type=MESH,
        )

    slot_here = lax.rem(root - leaf + n_leaf, n_leaf) - 1

    def seen_copy(block, slot):
        place = slice(0, height(block))
        return pltpu.make_async_remote_copy(
            src_ref=bulk_ref.at[block, place], dst_ref=seen_in.at[slot, SEEN.index(block), place],
            send_sem=gram_send.at[block], recv_sem=seen_recv.at[slot, SEEN.index(block)],
            device_id={"leaf": root, "top": after_top}, device_id_type=MESH,
        )

    def store(ref, block, value, symmetric):
        if symmetric:
            ref[block, :packed] = pack(value)
        else:
            ref[block] = value

    def piece_copy(block, number):
        a, b = peers[number]
        count, rows = parts(block), r // parts(block)
        there = beside(a, b)
        index = there["mid"] if count == n_mid else there["mid"] * n_top + there["top"]
        return pltpu.make_async_remote_copy(
            src_ref=raw_ref.at[PIECES.index(block), pl.ds(pl.multiple_of(index * rows, PANEL), rows)],
            dst_ref=piece_in.at[number, PIECES.index(block), slice(0, rows)],
            send_sem=piece_send.at[number, PIECES.index(block)], recv_sem=piece_recv.at[number, PIECES.index(block)],
            device_id=there, device_id_type=MESH,
        )

    def sharers(block):
        return [k for k, (a, b) in enumerate(peers) if b == 0 or parts(block) != n_mid]

    def own_place(block, group):
        rows = r // parts(block)
        index = mid if parts(block) == n_mid else mid * n_top + group
        return pl.ds(pl.multiple_of(index * rows, PANEL), rows)

    def share(block, value):
        raw_ref[PIECES.index(block)] = value
        for number in sharers(block):
            piece_copy(block, number).start()

    def join(block):
        k = PIECES.index(block)
        total = raw_ref[k, own_place(block, top)]
        for number in sharers(block):
            piece_copy(block, number).wait_recv()
            total = total + piece_in[number, k, : r // parts(block)]
        bulk_ref[block, : r // parts(block)] = total

    def give(block, value):
        store(bulk_ref, block, value, block in SYMMETRIC)

        if block not in LATER:
            @pl.when(is_other)
            def _():
                gram_copy(block, slot_here).start()

    prec, fine = fetch(0), fetch(1)
    solved_f = dot(prec, fine)
    s_ref[0] = solved_f
    gram_ff = dot(fine.T, solved_f)
    meet()
    give(FF, gram_ff)
    middle = fetch(2)
    mid_t = middle.T
    give(MF, dot(mid_t, solved_f))
    solved_m = dot(prec, middle)
    s_ref[1] = solved_m
    give(MM, dot(mid_t, solved_m))
    coarse = fetch(3)
    coarse_t = coarse.T
    give(CF, dot(coarse_t, solved_f))
    share(CM, dot(coarse_t, solved_m))
    solved_c = dot(prec, coarse)
    s_ref[2] = solved_c
    share(CC, dot(coarse_t, solved_c))
    obs = fetch(4)
    obs_t = obs.T
    share(YM, dot(obs_t, solved_m))
    share(YC, dot(obs_t, solved_c))
    give(YF, dot(obs_t, solved_f))
    s_ref[3] = dot(prec, obs)
    for k in range(5, 8):
        loads[k].wait()

    def gathered(block):
        place = slice(0, height(block))
        if block in PIECES:
            join(block)
        total = bulk_ref[block, place]
        for slot in range(n_leaf - 1):
            gram_copy(block, slot).wait_recv()
            total = total + gram_in[slot, block, place]
        return total

    def down_copy(block, slot, target):
        return pltpu.make_async_remote_copy(
            src_ref=down_ref.at[block], dst_ref=down_ref.at[block],
            send_sem=down_send.at[block, slot], recv_sem=down_recv.at[block],
            device_id={"leaf": target}, device_id_type=MESH,
        )

    def send_down(block, value):
        down_ref[block] = value
        for slot, exists in enumerate((root > 0, root < n_leaf - 1)):
            def go():
                down_copy(block, slot, root + 2 * slot - 1).start()

            if n_leaf > 2:
                go()
            else:
                pl.when(exists)(go)

    def spread_copy(block, step):
        return pltpu.make_async_remote_copy(
            src_ref=down_ref.at[block], dst_ref=down_ref.at[block],
            send_sem=spread_send.at[block - 3, step - 1], recv_sem=down_recv.at[block],
            device_id=leaf_at(step), device_id_type=MESH,
        )

    def send_all(block, value):
        down_ref[block] = value
        for step in leaf_steps:
            spread_copy(block, step).start()

    def pass_on(block):
        down_copy(block, 0, outer).wait_recv()
        down_copy(block, 0, outer).start()

    def seen(block):
        place = slice(0, height(block))
        for slot in range(n_leaf):
            seen_copy(block, slot).wait_recv()
        total = seen_in[0, SEEN.index(block), place]
        for slot in range(1, n_leaf):
            total = total + seen_in[slot, SEEN.index(block), place]
        return total

    def help_copy(number):
        return pltpu.make_async_remote_copy(
            src_ref=kept_ref.at[number], dst_ref=kept_ref.at[number],
            send_sem=help_send.at[number], recv_sem=help_recv.at[number],
            device_id={"top": after_top}, device_id_type=MESH,
        )

    def keep(number, value):
        kept_ref[number] = value
        help_copy(number).start()

    def answer_copy(number, step):
        target, arrival = (
            (down_ref.at[2], down_recv.at[2]),
            (last_ref.at[before_top, 1], last_recv.at[1, before_top]),
            (down_ref.at[4], down_recv.at[4]),
        )[number]
        return pltpu.make_async_remote_copy(
            src_ref=answer_ref.at[number], dst_ref=target,
            send_sem=answer_send.at[number, step], recv_sem=arrival,
            device_id={**leaf_at(step), "top": before_top}, device_id_type=MESH,
        )

    def send_answer(number, value):
        answer_ref[number] = value
        for step in [*leaf_steps, 0]:
            answer_copy(number, step).start()

    def cross_place(block):
        return slice(0, packed if block in (0, 3) else r)

    def cross_copy(block, step):
        return pltpu.make_async_remote_copy(
            src_ref=cross_ref.at[block, cross_place(block)], dst_ref=cross_in.at[step - 1, block, cross_place(block)],
            send_sem=cross_send.at[block, step - 1], recv_sem=cross_recv.at[block, step - 1],
            device_id={"mid": lax.rem(mid + step, n_mid)}, device_id_type=MESH,
        )

    def cross_start(block):
        for step in range(1, n_mid):
            cross_copy(block, step).start()

    def crossed(block):
        total = cross_ref[block, cross_place(block)]
        for step in range(1, n_mid):
            cross_copy(block, step).wait_recv()
            total = total + cross_in[step - 1, block, cross_place(block)]
        return total

    def corrected(raw, value):
        total_ref[...] = value
        piece, group = (seen(raw), before_top) if raw in SEEN else (gathered(raw), top)
        total_ref[own_place(raw, group)] = total_ref[own_place(raw, group)] + piece
        return total_ref[...]

    def last_place(block):
        return slice(0, r if block else packed)

    def last_copy(block, step):
        return pltpu.make_async_remote_copy(
            src_ref=last_ref.at[top, block, last_place(block)], dst_ref=last_ref.at[top, block, last_place(block)],
            send_sem=last_send.at[block, step - 1], recv_sem=last_recv.at[block, top],
            device_id=leaf_at(step), device_id_type=MESH,
        )

    def swap_copy(block, source, step):
        return pltpu.make_async_remote_copy(
            src_ref=last_ref.at[source, block, last_place(block)], dst_ref=last_ref.at[source, block, last_place(block)],
            send_sem=swap_send.at[block, step - 1], recv_sem=last_recv.at[block, source],
            device_id={"top": lax.rem(top + step, n_top)}, device_id_type=MESH,
        )

    def swap(block):
        for step in range(1, n_top):
            swap_copy(block, top, step).start()

    def send_last(block):
        for step in leaf_steps:
            last_copy(block, step).start()
        swap(block)

    def after_fine():
        s_ref[1] = s_ref[1] + dot_nt(s_ref[0], down_ref[0])
        s_ref[2] = s_ref[2] + dot_nt(s_ref[0], down_ref[1])
        s_ref[3] = s_ref[3] + dot_nt(s_ref[0], down_ref[2])

    @pl.when(is_root)
    def _():
        inverse = negated_inverse(a_ref, in_ref[5] + unpack(gathered(FF)))
        mf = gathered(MF)
        n_m = dot(mf, inverse)
        store(cross_ref, 0, unpack(gathered(MM)) + dot_nt(n_m, mf), True)
        cross_start(0)
        send_down(0, n_m)
        keep(0, inverse)
        keep(1, mf)
        cf = gathered(CF)
        n_c = dot(cf, inverse)
        keep(2, cf)
        lost = dot_nt(n_c, kept_ref[1:3].reshape(2 * r, r))
        cross_ref[1] = corrected(CM, lost[:, :r])
        cross_start(1)
        store(cross_ref, 3, corrected(CC, lost[:, r:]), True)
        cross_start(3)
        for block in SEEN:
            if block in PIECES:
                join(block)
            seen_copy(block, 0).start()
        send_down(1, n_c)

        inverse = negated_inverse(a_ref, in_ref[6] + unpack(crossed(0)))
        cm = crossed(1)
        q_c = dot(cm, inverse)
        store(last_ref.at[top], 0, unpack(crossed(3)) + dot_nt(q_c, cm), True)
        send_last(0)
        keep(3, inverse)
        keep(4, cm)
        send_all(3, q_c)

    @pl.when(is_other)
    def _():
        for block in LATER:
            if block in PIECES:
                join(block)
            if block in SEEN:
                seen_copy(block, slot_here + 1).start()
            else:
                gram_copy(block, slot_here).start()

    @pl.when(has_outer)
    def _():
        pass_on(0)

    @pl.when(is_helper)
    def _():
        for number in range(2):
            help_copy(number).wait_recv()
        n_y = dot(seen(YF), kept_ref[0])
        help_copy(2).wait_recv()
        lost = dot_nt(n_y, kept_ref[1:3].reshape(2 * r, r))
        cross_ref[2] = corrected(YM, lost[:, :r])
        cross_start(2)
        cross_ref[4] = corrected(YC, lost[:, r:])
        cross_start(4)
        send_answer(0, n_y)

    @pl.when(has_outer)
    def _():
        pass_on(1)

    @pl.when(is_helper)
    def _():
        for number in range(3, 5):
            help_copy(number).wait_recv()
        q_y = dot(crossed(2), kept_ref[3])
        send_answer(1, crossed(4) + dot_nt(q_y, kept_ref[4]))
        send_answer(2, q_y)

    @pl.when(is_other)
    def _():
        last_copy(0, 1).wait_recv()
        swap(0)

    @pl.when(is_other & ((outer < 0) | (outer >= n_leaf)))
    def _():
        down_copy(0, 0, outer).wait_recv()
        down_copy(1, 0, outer).wait_recv()

    down_copy(2, 0, outer).wait_recv()
    after_fine()

    def others_arrived(block):
        for step in range(1, n_top):
            swap_copy(block, lax.rem(top + step, n_top), step).wait_recv()

    others_arrived(0)
    coarse_sum = last_ref[0, 0, :packed]
    for t in range(1, n_top):
        coarse_sum = coarse_sum + last_ref[t, 0, :packed]

    def middle_of_inverse():
        last_copy(1, 1).wait_recv()
        swap(1)

    inverse = negated_inverse(a_ref, in_ref[7] + unpack(coarse_sum), middle_of_inverse)

    @pl.when(is_other)
    def _():
        spread_copy(3, 1).wait_recv()

    spread_copy(4, 1).wait_recv()
    others_arrived(1)
    right = last_ref[0, 1]
    for t in range(1, n_top):
        right = right + last_ref[t, 1]
    after = dot_nt(s_ref[1], down_ref[3:5].reshape(2 * r, r))
    out_ref[...] = s_ref[3] + after[:, r:] + dot_nt(s_ref[2] + after[:, :r], dot(right, inverse))

    for block in PIECES:
        for number in sharers(block):
            piece_copy(block, number).wait_send()
    for block in range(2):
        for step in range(1, n_top):
            swap_copy(block, top, step).wait_send()

    @pl.when(is_root)
    def _():
        for block in (0, 1, 3):
            for step in range(1, n_mid):
                cross_copy(block, step).wait_send()
        for step in leaf_steps:
            spread_copy(3, step).wait_send()
            last_copy(0, step).wait_send()
        for number in range(5):
            help_copy(number).wait_send()
        for block in SEEN:
            seen_copy(block, 0).wait_send()
        for block in range(2):
            for slot, exists in enumerate((root > 0, root < n_leaf - 1)):
                def done():
                    down_copy(block, slot, root + 2 * slot - 1).wait_send()

                if n_leaf > 2:
                    done()
                else:
                    pl.when(exists)(done)

    @pl.when(is_helper)
    def _():
        for block in (2, 4):
            for step in range(1, n_mid):
                cross_copy(block, step).wait_send()
        for number in range(3):
            for step in range(n_leaf):
                answer_copy(number, step).wait_send()

    @pl.when(is_other)
    def _():
        for block in range(9):
            gram_copy(block, slot_here).wait_send()

    @pl.when(has_outer)
    def _():
        for block in range(2):
            down_copy(block, 0, outer).wait_send()


def local(n_leaf, n_mid, n_top, *operands):
    blocks = [x.reshape(x.shape[-2:]) for x in operands]
    r = blocks[1].shape[1]
    f32 = jnp.float32
    dma = pltpu.SemaphoreType.DMA
    beside = max(n_mid * n_top - 1, 1)
    answer = pl.pallas_call(
        functools.partial(kernel, n_leaf, n_mid, n_top),
        out_shape=jax.ShapeDtypeStruct(blocks[-1].shape, f32),
        in_specs=[pl.BlockSpec(memory_space=pl.ANY)] * len(blocks),
        out_specs=pl.BlockSpec(memory_space=pltpu.VMEM),
        scratch_shapes=[
            pltpu.VMEM((8, r, r), f32),
            pltpu.VMEM((r + 2 * PANEL, r), f32),
            pltpu.VMEM((4, r, r), f32),
            pltpu.VMEM((4, r, r), f32),
            pltpu.VMEM((9, r, r), f32),
            pltpu.VMEM((beside, 4, r // n_mid, r), f32),
            pltpu.VMEM((n_leaf - 1, 9, r, r), f32),
            pltpu.VMEM((r, r), f32),
            pltpu.VMEM((5, r, r), f32),
            pltpu.VMEM((5, r, r), f32),
            pltpu.VMEM((5, r, r), f32),
            pltpu.VMEM((n_mid - 1, 5, r, r), f32),
            pltpu.VMEM((n_top, 2, r, r), f32),
            pltpu.VMEM((n_leaf, 3, r, r), f32),
            pltpu.VMEM((3, r, r), f32),
            dma((8,)),
            dma((beside, 4)), dma((beside, 4)),
            dma((9,)), dma((n_leaf - 1, 9)),
            dma((3, 2)), dma((5,)), dma((2, n_leaf - 1)),
            dma((5, n_mid - 1)), dma((5, n_mid - 1)),
            dma((2, n_leaf - 1)), dma((2, n_top)), dma((2, n_top - 1)),
            dma((n_leaf, 3)), dma((5,)), dma((5,)), dma((3, n_leaf)),
        ],
        compiler_params=pltpu.CompilerParams(
            collective_id=0, has_side_effects=True, vmem_limit_bytes=VMEM_ROOM - 3 * r * blocks[-1].shape[1] * 2,
        ),
    )(*blocks)
    return answer[None, None, None]


def solution(mesh):
    spread = P(("parts", "leaf"), "mid", "top", None, None)
    sizes = (mesh.shape["leaf"], mesh.shape["mid"], mesh.shape["top"])
    return jax.shard_map(
        functools.partial(local, *sizes),
        mesh=mesh,
        in_specs=(spread, spread, spread, spread, P(), P(), P(), spread),
        out_specs=spread,
        check_vma=False,
    )
```

```python
import functools

import jax
import jax.numpy as jnp
from jax import lax
from jax.experimental import pallas as pl
from jax.experimental.pallas import tpu as pltpu
from jax.sharding import PartitionSpec as P

MESH = pl.DeviceIdType.MESH
PANEL = 8
VMEM_ROOM = 56_558_000


def dot(left_hand, right_side):
    return jnp.dot(
        left_hand, right_side, precision=lax.Precision.HIGHEST, preferred_element_type=jnp.float32
    )


def split3(x):
    high = x.astype(jnp.bfloat16).astype(jnp.float32)
    rest = x - high
    mid = rest.astype(jnp.bfloat16).astype(jnp.float32)
    low = (rest - mid).astype(jnp.bfloat16).astype(jnp.float32)
    return high, mid, low


def spread_panel(panel):
    p1, p2, p3 = split3(panel)
    return jnp.concatenate([p1, p1, p2, p2, p1, p3], axis=0).T.astype(jnp.bfloat16)


def rank_update(spread, scaled):
    r1, r2, r3 = split3(scaled)
    right_side = jnp.concatenate([r1, r2, r1, r2, r3, r1], axis=0).astype(jnp.bfloat16)
    return jnp.dot(spread, right_side, preferred_element_type=jnp.float32)


def negated_inverse(a_ref, matrix, between=None):
    size = matrix.shape[0]
    zero = jnp.zeros((PANEL, size), jnp.float32)
    a_ref[pl.ds(0, PANEL), :] = zero
    a_ref[pl.ds(PANEL, size), :] = matrix
    a_ref[pl.ds(PANEL + size, PANEL), :] = zero
    lane = lax.broadcasted_iota(jnp.int32, (PANEL, size), 1)
    sub = lax.broadcasted_iota(jnp.int32, (PANEL, size), 0)
    lane_full = lax.broadcasted_iota(jnp.int32, (size, size), 1)

    def lanes(block, index):
        picked = jnp.where(lane == index, block, 0.0)
        return jnp.broadcast_to(jnp.sum(picked, axis=1, keepdims=True), block.shape)

    def row_of(block, i):
        return jnp.broadcast_to(block[i : i + 1], block.shape)

    def apply(k, spread, scaled):
        inside = (lane_full >= k * PANEL) & (lane_full < (k + 1) * PANEL)
        current = a_ref[pl.ds(PANEL, size), :]
        a_ref[pl.ds(PANEL, size), :] = jnp.where(inside, 0.0, current) - rank_update(spread, scaled)
        a_ref[pl.ds(pl.multiple_of((k + 1) * PANEL, PANEL), PANEL), :] = scaled

    def body(k, carry):
        spread_before, scaled_before, panel = carry
        apply(k - 1, spread_before, scaled_before)
        inside = (lane >= k * PANEL) & (lane < (k + 1) * PANEL)
        cols = [lanes(panel, k * PANEL + j) for j in range(PANEL)]
        ahead = (k + 1) * PANEL + sub
        below = [lanes(row_of(panel, j), ahead) for j in range(PANEL)]
        spread = spread_panel(panel)
        following = a_ref[pl.ds(pl.multiple_of((k + 2) * PANEL, PANEL), PANEL), :]
        x = jnp.where(inside, jnp.where(lane - k * PANEL == sub, 1.0, 0.0), panel)
        gone = jnp.zeros_like(x)
        scale = gone
        for i in range(PANEL):
            pivot = 1.0 / row_of(cols[i], i)
            here = sub == i
            factor = jnp.where(here, 0.0, cols[i])
            row = row_of(x, i)
            across, down = factor * pivot, below[i] * pivot
            for j in range(i + 1, PANEL):
                entry = row_of(cols[j], i)
                if j == i + 1:
                    cols[j] = cols[j] - (factor * entry) * pivot
                else:
                    cols[j] = cols[j] - across * entry
                below[j] = below[j] - down * entry
            x = x - across * row
            gone = gone + down * row
            scale = jnp.where(here, pivot, scale)
        x = x * scale
        return spread, jnp.where(inside, -x, x), jnp.where(inside, gone, following - gone)

    steps = size // PANEL
    carry = (spread_panel(zero), zero, matrix[:PANEL])
    if between is None:
        spread, scaled, _ = lax.fori_loop(0, steps, body, carry)
    else:
        carry = lax.fori_loop(0, steps // 2, body, carry)
        between()
        spread, scaled, _ = lax.fori_loop(steps // 2, steps, body, carry)
    apply(steps - 1, spread, scaled)
    return a_ref[pl.ds(PANEL, size), :]


def dot_nt(left_hand, right_rows):
    return lax.dot_general(
        left_hand, right_rows, (((1,), (1,)), ((), ())),
        precision=lax.Precision.HIGHEST, preferred_element_type=jnp.float32,
    )


def pack(matrix):
    half, size = matrix.shape[0] // 2, matrix.shape[1]
    lane = lax.broadcasted_iota(jnp.int32, (PANEL, size), 1)
    blocks = [matrix[:PANEL]]
    for start in range(PANEL, half + 1, PANEL):
        moved = pltpu.roll(matrix[size - start : size - start + PANEL], start, 1)
        blocks.append(moved if start == half else jnp.where(lane < start, moved, matrix[start : start + PANEL]))
    return jnp.concatenate(blocks, axis=0)


def unpack(packed):
    half, size = packed.shape[0] - PANEL, packed.shape[1]
    bottom = [pltpu.roll(packed[start : start + PANEL], size - start, 1) for start in range(half, 0, -PANEL)]
    return jnp.concatenate([packed[:half], *bottom], axis=0)


FF, MF, MM, CF, CM, YF, YM, CC, YC = range(9)
SYMMETRIC = (FF, MM)
LATER = (CM, CC, YF, YM, YC)
PIECES = (CM, YM, CC, YC)
SEEN = (YF, YM, YC)


def kernel(
    n_leaf, n_mid, n_top,
    prec_hbm, fine_hbm, mid_hbm, coarse_hbm, core_fine_hbm, core_mid_hbm, core_coarse_hbm, obs_hbm,
    out_ref,
    in_ref, a_ref, s_ref, raw_ref, bulk_ref, piece_in, gram_in, total_ref, kept_ref, down_ref, cross_ref, cross_in, last_ref, seen_in, answer_ref,
    in_sem, piece_send, piece_recv, gram_send, gram_recv, down_send, down_recv, spread_send,
    cross_send, cross_recv, last_send, last_recv, swap_send, seen_recv, help_send, help_recv, answer_send,
):
    r = bulk_ref.shape[1]
    packed = r // 2 + PANEL
    leaf, mid, top = lax.axis_index("leaf"), lax.axis_index("mid"), lax.axis_index("top")
    low, high = (n_leaf - 1) // 2, n_leaf // 2

    def root_of(index):
        return low + lax.rem(index, 2) * (high - low)

    root = root_of(top)
    after_top, before_top = lax.rem(top + 1, n_top), lax.rem(top + n_top - 1, n_top)
    is_helper = leaf == root_of(before_top)
    is_root = leaf == root
    is_other = leaf != root
    side = (leaf > root).astype(jnp.int32)
    inner, outer = leaf + 1 - 2 * side, leaf - 1 + 2 * side
    has_outer = is_other & (outer >= 0) & (outer < n_leaf)
    inner_is_other = is_other & (inner != root)
    barrier = pltpu.get_barrier_semaphore()

    def greet(device):
        pl.semaphore_signal(barrier, inc=1, device_id=device, device_id_type=MESH)

    leaf_steps = sorted(range(1, n_leaf), key=lambda step: (abs(2 * step - n_leaf), step))
    peers = [(a, b) for a in range(n_mid) for b in range(n_top) if (a, b) != (0, 0)]

    def beside(a, b):
        return {"mid": lax.rem(mid + a, n_mid), "top": lax.rem(top + b, n_top)}

    def leaf_at(step):
        return {"leaf": lax.rem(leaf + step, n_leaf)}

    for a, b in peers:
        greet(beside(a, b))

    @pl.when(is_root)
    def _():
        for step in leaf_steps:
            greet(leaf_at(step))

    @pl.when(is_other)
    def _():
        greet({"leaf": root})

        greet({"leaf": root, "top": after_top})

    @pl.when(is_helper)
    def _():
        for step in leaf_steps:
            greet({**leaf_at(step), "top": before_top})

    @pl.when(has_outer)
    def _():
        greet({"leaf": outer})

    @pl.when(inner_is_other)
    def _():
        greet({"leaf": inner})

    sources = [prec_hbm, fine_hbm, mid_hbm, coarse_hbm, obs_hbm, core_fine_hbm, core_mid_hbm, core_coarse_hbm]
    loads = [pltpu.make_async_copy(src, in_ref.at[k], in_sem.at[k]) for k, src in enumerate(sources)]
    for load in loads:
        load.start()

    def fetch(k):
        loads[k].wait()
        return in_ref[k]

    def meet():
        around = jnp.where(is_root, n_leaf - 1, 2 + has_outer.astype(jnp.int32) + inner_is_other.astype(jnp.int32))
        helped = jnp.where(is_helper, n_leaf - 1, 0)
        pl.semaphore_wait(barrier, len(peers) + around + helped)

    def parts(block):
        return n_mid if block in (CM, YM) else n_mid * n_top

    def height(block):
        if block in SYMMETRIC:
            return packed
        return r // parts(block) if block in PIECES else r

    def gram_copy(block, slot):
        place = slice(0, height(block))
        return pltpu.make_async_remote_copy(
            src_ref=bulk_ref.at[block, place], dst_ref=gram_in.at[slot, block, place],
            send_sem=gram_send.at[block], recv_sem=gram_recv.at[slot, block],
            device_id={"leaf": root}, device_id_type=MESH,
        )

    slot_here = lax.rem(root - leaf + n_leaf, n_leaf) - 1

    def seen_copy(block, slot):
        place = slice(0, height(block))
        return pltpu.make_async_remote_copy(
            src_ref=bulk_ref.at[block, place], dst_ref=seen_in.at[slot, SEEN.index(block), place],
            send_sem=gram_send.at[block], recv_sem=seen_recv.at[slot, SEEN.index(block)],
            device_id={"leaf": root, "top": after_top}, device_id_type=MESH,
        )

    def store(ref, block, value, symmetric):
        if symmetric:
            ref[block, :packed] = pack(value)
        else:
            ref[block] = value

    def piece_copy(block, number):
        a, b = peers[number]
        count, rows = parts(block), r // parts(block)
        there = beside(a, b)
        index = there["mid"] if count == n_mid else there["mid"] * n_top + there["top"]
        return pltpu.make_async_remote_copy(
            src_ref=raw_ref.at[PIECES.index(block), pl.ds(pl.multiple_of(index * rows, PANEL), rows)],
            dst_ref=piece_in.at[number, PIECES.index(block), slice(0, rows)],
            send_sem=piece_send.at[number, PIECES.index(block)], recv_sem=piece_recv.at[number, PIECES.index(block)],
            device_id=there, device_id_type=MESH,
        )

    def sharers(block):
        return [k for k, (a, b) in enumerate(peers) if b == 0 or parts(block) != n_mid]

    def own_place(block, group):
        rows = r // parts(block)
        index = mid if parts(block) == n_mid else mid * n_top + group
        return pl.ds(pl.multiple_of(index * rows, PANEL), rows)

    def share(block, value):
        raw_ref[PIECES.index(block)] = value
        for number in sharers(block):
            piece_copy(block, number).start()

    def join(block):
        k = PIECES.index(block)
        total = raw_ref[k, own_place(block, top)]
        for number in sharers(block):
            piece_copy(block, number).wait_recv()
            total = total + piece_in[number, k, : r // parts(block)]
        bulk_ref[block, : r // parts(block)] = total

    def give(block, value):
        store(bulk_ref, block, value, block in SYMMETRIC)

        if block not in LATER:
            @pl.when(is_other)
            def _():
                gram_copy(block, slot_here).start()

    prec, fine = fetch(0), fetch(1)
    solved_f = dot(prec, fine)
    s_ref[0] = solved_f
    gram_ff = dot(fine.T, solved_f)
    meet()
    give(FF, gram_ff)
    middle = fetch(2)
    mid_t = middle.T
    give(MF, dot(mid_t, solved_f))
    solved_m = dot(prec, middle)
    s_ref[1] = solved_m
    give(MM, dot(mid_t, solved_m))
    coarse = fetch(3)
    coarse_t = coarse.T
    give(CF, dot(coarse_t, solved_f))
    share(CM, dot(coarse_t, solved_m))
    solved_c = dot(prec, coarse)
    s_ref[2] = solved_c
    share(CC, dot(coarse_t, solved_c))
    obs = fetch(4)
    obs_t = obs.T
    share(YM, dot(obs_t, solved_m))
    share(YC, dot(obs_t, solved_c))
    give(YF, dot(obs_t, solved_f))
    s_ref[3] = dot(prec, obs)
    for k in range(5, 8):
        loads[k].wait()

    def gathered(block):
        place = slice(0, height(block))
        if block in PIECES:
            join(block)
        total = bulk_ref[block, place]
        for slot in range(n_leaf - 1):
            gram_copy(block, slot).wait_recv()
            total = total + gram_in[slot, block, place]
        return total

    def down_copy(block, slot, target):
        return pltpu.make_async_remote_copy(
            src_ref=down_ref.at[block], dst_ref=down_ref.at[block],
            send_sem=down_send.at[block, slot], recv_sem=down_recv.at[block],
            device_id={"leaf": target}, device_id_type=MESH,
        )

    def send_down(block, value):
        down_ref[block] = value
        for slot, exists in enumerate((root > 0, root < n_leaf - 1)):
            def go():
                down_copy(block, slot, root + 2 * slot - 1).start()

            if n_leaf > 2:
                go()
            else:
                pl.when(exists)(go)

    def spread_copy(block, step):
        return pltpu.make_async_remote_copy(
            src_ref=down_ref.at[block], dst_ref=down_ref.at[block],
            send_sem=spread_send.at[block - 3, step - 1], recv_sem=down_recv.at[block],
            device_id=leaf_at(step), device_id_type=MESH,
        )

    def send_all(block, value):
        down_ref[block] = value
        for step in leaf_steps:
            spread_copy(block, step).start()

    def pass_on(block):
        down_copy(block, 0, outer).wait_recv()
        down_copy(block, 0, outer).start()

    def seen(block):
        place = slice(0, height(block))
        for slot in range(n_leaf):
            seen_copy(block, slot).wait_recv()
        total = seen_in[0, SEEN.index(block), place]
        for slot in range(1, n_leaf):
            total = total + seen_in[slot, SEEN.index(block), place]
        return total

    def help_copy(number):
        return pltpu.make_async_remote_copy(
            src_ref=kept_ref.at[number], dst_ref=kept_ref.at[number],
            send_sem=help_send.at[number], recv_sem=help_recv.at[number],
            device_id={"top": after_top}, device_id_type=MESH,
        )

    def keep(number, value):
        kept_ref[number] = value
        help_copy(number).start()

    def answer_copy(number, step):
        target, arrival = (
            (down_ref.at[2], down_recv.at[2]),
            (last_ref.at[before_top, 1], last_recv.at[1, before_top]),
            (down_ref.at[4], down_recv.at[4]),
        )[number]
        return pltpu.make_async_remote_copy(
            src_ref=answer_ref.at[number], dst_ref=target,
            send_sem=answer_send.at[number, step], recv_sem=arrival,
            device_id={**leaf_at(step), "top": before_top}, device_id_type=MESH,
        )

    def send_answer(number, value):
        answer_ref[number] = value
        for step in [*leaf_steps, 0]:
            answer_copy(number, step).start()

    def cross_place(block):
        return slice(0, packed if block in (0, 3) else r)

    def cross_copy(block, step):
        return pltpu.make_async_remote_copy(
            src_ref=cross_ref.at[block, cross_place(block)], dst_ref=cross_in.at[step - 1, block, cross_place(block)],
            send_sem=cross_send.at[block, step - 1], recv_sem=cross_recv.at[block, step - 1],
            device_id={"mid": lax.rem(mid + step, n_mid)}, device_id_type=MESH,
        )

    def cross_start(block):
        for step in range(1, n_mid):
            cross_copy(block, step).start()

    def crossed(block):
        total = cross_ref[block, cross_place(block)]
        for step in range(1, n_mid):
            cross_copy(block, step).wait_recv()
            total = total + cross_in[step - 1, block, cross_place(block)]
        return total

    def corrected(raw, value):
        total_ref[...] = value
        piece, group = (seen(raw), before_top) if raw in SEEN else (gathered(raw), top)
        total_ref[own_place(raw, group)] = total_ref[own_place(raw, group)] + piece
        return total_ref[...]

    def last_place(block):
        return slice(0, r if block else packed)

    def last_copy(block, step):
        return pltpu.make_async_remote_copy(
            src_ref=last_ref.at[top, block, last_place(block)], dst_ref=last_ref.at[top, block, last_place(block)],
            send_sem=last_send.at[block, step - 1], recv_sem=last_recv.at[block, top],
            device_id=leaf_at(step), device_id_type=MESH,
        )

    def swap_copy(block, source, step):
        return pltpu.make_async_remote_copy(
            src_ref=last_ref.at[source, block, last_place(block)], dst_ref=last_ref.at[source, block, last_place(block)],
            send_sem=swap_send.at[block, step - 1], recv_sem=last_recv.at[block, source],
            device_id={"top": lax.rem(top + step, n_top)}, device_id_type=MESH,
        )

    def swap(block):
        for step in range(1, n_top):
            swap_copy(block, top, step).start()

    def send_last(block):
        for step in leaf_steps:
            last_copy(block, step).start()
        swap(block)

    def after_fine():
        s_ref[1] = s_ref[1] + dot_nt(s_ref[0], down_ref[0])
        s_ref[2] = s_ref[2] + dot_nt(s_ref[0], down_ref[1])
        s_ref[3] = s_ref[3] + dot_nt(s_ref[0], down_ref[2])

    @pl.when(is_root)
    def _():
        inverse = negated_inverse(a_ref, in_ref[5] + unpack(gathered(FF)))
        mf = gathered(MF)
        n_m = dot(mf, inverse)
        store(cross_ref, 0, unpack(gathered(MM)) + dot_nt(n_m, mf), True)
        cross_start(0)
        send_down(0, n_m)
        keep(0, inverse)
        keep(1, mf)
        cf = gathered(CF)
        n_c = dot(cf, inverse)
        keep(2, cf)
        lost = dot_nt(n_c, kept_ref[1:3].reshape(2 * r, r))
        cross_ref[1] = corrected(CM, lost[:, :r])
        cross_start(1)
        store(cross_ref, 3, corrected(CC, lost[:, r:]), True)
        cross_start(3)
        send_down(1, n_c)
        for block in SEEN:
            if block in PIECES:
                join(block)
            seen_copy(block, 0).start()

        inverse = negated_inverse(a_ref, in_ref[6] + unpack(crossed(0)))
        cm = crossed(1)
        q_c = dot(cm, inverse)
        store(last_ref.at[top], 0, unpack(crossed(3)) + dot_nt(q_c, cm), True)
        send_last(0)
        keep(3, inverse)
        keep(4, cm)
        send_all(3, q_c)

    @pl.when(is_other)
    def _():
        for block in LATER:
            if block in PIECES:
                join(block)
            if block in SEEN:
                seen_copy(block, slot_here + 1).start()
            else:
                gram_copy(block, slot_here).start()

    @pl.when(has_outer)
    def _():
        pass_on(0)

    @pl.when(is_helper)
    def _():
        for number in range(2):
            help_copy(number).wait_recv()
        n_y = dot(seen(YF), kept_ref[0])
        send_answer(0, n_y)
        help_copy(2).wait_recv()
        lost = dot_nt(n_y, kept_ref[1:3].reshape(2 * r, r))
        cross_ref[2] = corrected(YM, lost[:, :r])
        cross_start(2)
        cross_ref[4] = corrected(YC, lost[:, r:])
        cross_start(4)

    @pl.when(has_outer)
    def _():
        pass_on(1)

    @pl.when(is_helper)
    def _():
        for number in range(3, 5):
            help_copy(number).wait_recv()
        q_y = dot(crossed(2), kept_ref[3])
        send_answer(1, crossed(4) + dot_nt(q_y, kept_ref[4]))
        send_answer(2, q_y)

    @pl.when(is_other)
    def _():
        last_copy(0, 1).wait_recv()
        swap(0)

    @pl.when(is_other & ((outer < 0) | (outer >= n_leaf)))
    def _():
        down_copy(0, 0, outer).wait_recv()
        down_copy(1, 0, outer).wait_recv()

    down_copy(2, 0, outer).wait_recv()
    after_fine()

    def others_arrived(block):
        for step in range(1, n_top):
            swap_copy(block, lax.rem(top + step, n_top), step).wait_recv()

    others_arrived(0)
    coarse_sum = last_ref[0, 0, :packed]
    for t in range(1, n_top):
        coarse_sum = coarse_sum + last_ref[t, 0, :packed]

    def middle_of_inverse():
        last_copy(1, 1).wait_recv()
        swap(1)

    inverse = negated_inverse(a_ref, in_ref[7] + unpack(coarse_sum), middle_of_inverse)

    @pl.when(is_other)
    def _():
        spread_copy(3, 1).wait_recv()

    spread_copy(4, 1).wait_recv()
    others_arrived(1)
    right = last_ref[0, 1]
    for t in range(1, n_top):
        right = right + last_ref[t, 1]
    after = dot_nt(s_ref[1], down_ref[3:5].reshape(2 * r, r))
    out_ref[...] = s_ref[3] + after[:, r:] + dot_nt(s_ref[2] + after[:, :r], dot(right, inverse))

    for block in PIECES:
        for number in sharers(block):
            piece_copy(block, number).wait_send()
    for block in range(2):
        for step in range(1, n_top):
            swap_copy(block, top, step).wait_send()

    @pl.when(is_root)
    def _():
        for block in (0, 1, 3):
            for step in range(1, n_mid):
                cross_copy(block, step).wait_send()
        for step in leaf_steps:
            spread_copy(3, step).wait_send()
            last_copy(0, step).wait_send()
        for number in range(5):
            help_copy(number).wait_send()
        for block in SEEN:
            seen_copy(block, 0).wait_send()
        for block in range(2):
            for slot, exists in enumerate((root > 0, root < n_leaf - 1)):
                def done():
                    down_copy(block, slot, root + 2 * slot - 1).wait_send()

                if n_leaf > 2:
                    done()
                else:
                    pl.when(exists)(done)

    @pl.when(is_helper)
    def _():
        for block in (2, 4):
            for step in range(1, n_mid):
                cross_copy(block, step).wait_send()
        for number in range(3):
            for step in range(n_leaf):
                answer_copy(number, step).wait_send()

    @pl.when(is_other)
    def _():
        for block in range(9):
            gram_copy(block, slot_here).wait_send()

    @pl.when(has_outer)
    def _():
        for block in range(2):
            down_copy(block, 0, outer).wait_send()


def local(n_leaf, n_mid, n_top, *operands):
    blocks = [x.reshape(x.shape[-2:]) for x in operands]
    r = blocks[1].shape[1]
    f32 = jnp.float32
    dma = pltpu.SemaphoreType.DMA
    beside = max(n_mid * n_top - 1, 1)
    answer = pl.pallas_call(
        functools.partial(kernel, n_leaf, n_mid, n_top),
        out_shape=jax.ShapeDtypeStruct(blocks[-1].shape, f32),
        in_specs=[pl.BlockSpec(memory_space=pl.ANY)] * len(blocks),
        out_specs=pl.BlockSpec(memory_space=pltpu.VMEM),
        scratch_shapes=[
            pltpu.VMEM((8, r, r), f32),
            pltpu.VMEM((r + 2 * PANEL, r), f32),
            pltpu.VMEM((4, r, r), f32),
            pltpu.VMEM((4, r, r), f32),
            pltpu.VMEM((9, r, r), f32),
            pltpu.VMEM((beside, 4, r // n_mid, r), f32),
            pltpu.VMEM((n_leaf - 1, 9, r, r), f32),
            pltpu.VMEM((r, r), f32),
            pltpu.VMEM((5, r, r), f32),
            pltpu.VMEM((5, r, r), f32),
            pltpu.VMEM((5, r, r), f32),
            pltpu.VMEM((n_mid - 1, 5, r, r), f32),
            pltpu.VMEM((n_top, 2, r, r), f32),
            pltpu.VMEM((n_leaf, 3, r, r), f32),
            pltpu.VMEM((3, r, r), f32),
            dma((8,)),
            dma((beside, 4)), dma((beside, 4)),
            dma((9,)), dma((n_leaf - 1, 9)),
            dma((3, 2)), dma((5,)), dma((2, n_leaf - 1)),
            dma((5, n_mid - 1)), dma((5, n_mid - 1)),
            dma((2, n_leaf - 1)), dma((2, n_top)), dma((2, n_top - 1)),
            dma((n_leaf, 3)), dma((5,)), dma((5,)), dma((3, n_leaf)),
        ],
        compiler_params=pltpu.CompilerParams(
            collective_id=0, has_side_effects=True, vmem_limit_bytes=VMEM_ROOM - 3 * r * blocks[-1].shape[1] * 2,
        ),
    )(*blocks)
    return answer[None, None, None]


def solution(mesh):
    spread = P(("parts", "leaf"), "mid", "top", None, None)
    sizes = (mesh.shape["leaf"], mesh.shape["mid"], mesh.shape["top"])
    return jax.shard_map(
        functools.partial(local, *sizes),
        mesh=mesh,
        in_specs=(spread, spread, spread, spread, P(), P(), P(), spread),
        out_specs=spread,
        check_vma=False,
    )
```

```python
import functools

import jax
import jax.numpy as jnp
from jax import lax
from jax.experimental import pallas as pl
from jax.experimental.pallas import tpu as pltpu
from jax.sharding import PartitionSpec as P

MESH = pl.DeviceIdType.MESH
PANEL = 8
VMEM_ROOM = 56_558_000


def dot(left_hand, right_side):
    return jnp.dot(
        left_hand, right_side, precision=lax.Precision.HIGHEST, preferred_element_type=jnp.float32
    )


def split3(x):
    high = x.astype(jnp.bfloat16).astype(jnp.float32)
    rest = x - high
    mid = rest.astype(jnp.bfloat16).astype(jnp.float32)
    low = (rest - mid).astype(jnp.bfloat16).astype(jnp.float32)
    return high, mid, low


def spread_panel(panel):
    p1, p2, p3 = split3(panel)
    return jnp.concatenate([p1, p1, p2, p2, p1, p3], axis=0).T.astype(jnp.bfloat16)


def rank_update(spread, scaled):
    r1, r2, r3 = split3(scaled)
    right_side = jnp.concatenate([r1, r2, r1, r2, r3, r1], axis=0).astype(jnp.bfloat16)
    return jnp.dot(spread, right_side, preferred_element_type=jnp.float32)


def negated_inverse(a_ref, matrix, between=None):
    size = matrix.shape[0]
    zero = jnp.zeros((PANEL, size), jnp.float32)
    a_ref[pl.ds(0, PANEL), :] = zero
    a_ref[pl.ds(PANEL, size), :] = matrix
    a_ref[pl.ds(PANEL + size, PANEL), :] = zero
    lane = lax.broadcasted_iota(jnp.int32, (PANEL, size), 1)
    sub = lax.broadcasted_iota(jnp.int32, (PANEL, size), 0)
    lane_full = lax.broadcasted_iota(jnp.int32, (size, size), 1)

    def lanes(block, index):
        picked = jnp.where(lane == index, block, 0.0)
        return jnp.broadcast_to(jnp.sum(picked, axis=1, keepdims=True), block.shape)

    def row_of(block, i):
        return jnp.broadcast_to(block[i : i + 1], block.shape)

    def apply(k, spread, scaled):
        inside = (lane_full >= k * PANEL) & (lane_full < (k + 1) * PANEL)
        current = a_ref[pl.ds(PANEL, size), :]
        a_ref[pl.ds(PANEL, size), :] = jnp.where(inside, 0.0, current) - rank_update(spread, scaled)
        a_ref[pl.ds(pl.multiple_of((k + 1) * PANEL, PANEL), PANEL), :] = scaled

    def body(k, carry):
        spread_before, scaled_before, panel = carry
        apply(k - 1, spread_before, scaled_before)
        inside = (lane >= k * PANEL) & (lane < (k + 1) * PANEL)
        cols = [lanes(panel, k * PANEL + j) for j in range(PANEL)]
        ahead = (k + 1) * PANEL + sub
        below = [lanes(row_of(panel, j), ahead) for j in range(PANEL)]
        spread = spread_panel(panel)
        following = a_ref[pl.ds(pl.multiple_of((k + 2) * PANEL, PANEL), PANEL), :]
        x = jnp.where(inside, jnp.where(lane - k * PANEL == sub, 1.0, 0.0), panel)
        gone = jnp.zeros_like(x)
        scale = gone
        for i in range(PANEL):
            pivot = 1.0 / row_of(cols[i], i)
            here = sub == i
            factor = jnp.where(here, 0.0, cols[i])
            row = row_of(x, i)
            across, down = factor * pivot, below[i] * pivot
            for j in range(i + 1, PANEL):
                entry = row_of(cols[j], i)
                if j == i + 1:
                    cols[j] = cols[j] - (factor * entry) * pivot
                else:
                    cols[j] = cols[j] - across * entry
                below[j] = below[j] - down * entry
            x = x - across * row
            gone = gone + down * row
            scale = jnp.where(here, pivot, scale)
        x = x * scale
        return spread, jnp.where(inside, -x, x), jnp.where(inside, gone, following - gone)

    steps = size // PANEL
    carry = (spread_panel(zero), zero, matrix[:PANEL])
    if between is None:
        spread, scaled, _ = lax.fori_loop(0, steps, body, carry)
    else:
        carry = lax.fori_loop(0, steps // 2, body, carry)
        between()
        spread, scaled, _ = lax.fori_loop(steps // 2, steps, body, carry)
    apply(steps - 1, spread, scaled)
    return a_ref[pl.ds(PANEL, size), :]


def dot_nt(left_hand, right_rows):
    return lax.dot_general(
        left_hand, right_rows, (((1,), (1,)), ((), ())),
        precision=lax.Precision.HIGHEST, preferred_element_type=jnp.float32,
    )


def pack(matrix):
    half, size = matrix.shape[0] // 2, matrix.shape[1]
    lane = lax.broadcasted_iota(jnp.int32, (PANEL, size), 1)
    blocks = [matrix[:PANEL]]
    for start in range(PANEL, half + 1, PANEL):
        moved = pltpu.roll(matrix[size - start : size - start + PANEL], start, 1)
        blocks.append(moved if start == half else jnp.where(lane < start, moved, matrix[start : start + PANEL]))
    return jnp.concatenate(blocks, axis=0)


def unpack(packed):
    half, size = packed.shape[0] - PANEL, packed.shape[1]
    bottom = [pltpu.roll(packed[start : start + PANEL], size - start, 1) for start in range(half, 0, -PANEL)]
    return jnp.concatenate([packed[:half], *bottom], axis=0)


FF, MF, MM, CF, CM, YF, YM, CC, YC = range(9)
SYMMETRIC = (FF, MM)
LATER = (CM, CC, YF, YM, YC)
PIECES = (CM, YM, CC, YC)
SEEN = (YF, YM, YC)


def kernel(
    n_leaf, n_mid, n_top,
    prec_hbm, fine_hbm, mid_hbm, coarse_hbm, core_fine_hbm, core_mid_hbm, core_coarse_hbm, obs_hbm,
    out_ref,
    in_ref, a_ref, s_ref, raw_ref, bulk_ref, piece_in, gram_in, total_ref, kept_ref, down_ref, cross_ref, cross_in, last_ref, seen_in, answer_ref,
    in_sem, piece_send, piece_recv, gram_send, gram_recv, down_send, down_recv, spread_send,
    cross_send, cross_recv, last_send, last_recv, swap_send, seen_recv, help_send, help_recv, answer_send,
):
    r = bulk_ref.shape[1]
    packed = r // 2 + PANEL
    leaf, mid, top = lax.axis_index("leaf"), lax.axis_index("mid"), lax.axis_index("top")
    low, high = (n_leaf - 1) // 2, n_leaf // 2

    def root_of(index):
        return low + lax.rem(index, 2) * (high - low)

    root = root_of(top)
    after_top, before_top = lax.rem(top + 1, n_top), lax.rem(top + n_top - 1, n_top)
    is_helper = leaf == root_of(before_top)
    is_root = leaf == root
    is_other = leaf != root
    side = (leaf > root).astype(jnp.int32)
    inner, outer = leaf + 1 - 2 * side, leaf - 1 + 2 * side
    has_outer = is_other & (outer >= 0) & (outer < n_leaf)
    inner_is_other = is_other & (inner != root)
    barrier = pltpu.get_barrier_semaphore()

    def greet(device):
        pl.semaphore_signal(barrier, inc=1, device_id=device, device_id_type=MESH)

    leaf_steps = sorted(range(1, n_leaf), key=lambda step: (abs(2 * step - n_leaf), step))
    peers = [(a, b) for a in range(n_mid) for b in range(n_top) if (a, b) != (0, 0)]

    def beside(a, b):
        return {"mid": lax.rem(mid + a, n_mid), "top": lax.rem(top + b, n_top)}

    def leaf_at(step):
        return {"leaf": lax.rem(leaf + step, n_leaf)}

    for a, b in peers:
        greet(beside(a, b))

    @pl.when(is_root)
    def _():
        for step in leaf_steps:
            greet(leaf_at(step))

    @pl.when(is_other)
    def _():
        greet({"leaf": root})

        greet({"leaf": root, "top": after_top})

    @pl.when(is_helper)
    def _():
        for step in leaf_steps:
            greet({**leaf_at(step), "top": before_top})

    @pl.when(has_outer)
    def _():
        greet({"leaf": outer})

    @pl.when(inner_is_other)
    def _():
        greet({"leaf": inner})

    sources = [prec_hbm, fine_hbm, mid_hbm, coarse_hbm, obs_hbm, core_fine_hbm, core_mid_hbm, core_coarse_hbm]
    loads = [pltpu.make_async_copy(src, in_ref.at[k], in_sem.at[k]) for k, src in enumerate(sources)]
    for load in loads:
        load.start()

    def fetch(k):
        loads[k].wait()
        return in_ref[k]

    def meet():
        around = jnp.where(is_root, n_leaf - 1, 2 + has_outer.astype(jnp.int32) + inner_is_other.astype(jnp.int32))
        helped = jnp.where(is_helper, n_leaf - 1, 0)
        pl.semaphore_wait(barrier, len(peers) + around + helped)

    def parts(block):
        return n_mid if block in (CM, YM) else n_mid * n_top

    def height(block):
        if block in SYMMETRIC:
            return packed
        return r // parts(block) if block in PIECES else r

    def gram_copy(block, slot):
        place = slice(0, height(block))
        return pltpu.make_async_remote_copy(
            src_ref=bulk_ref.at[block, place], dst_ref=gram_in.at[slot, block, place],
            send_sem=gram_send.at[block], recv_sem=gram_recv.at[slot, block],
            device_id={"leaf": root}, device_id_type=MESH,
        )

    slot_here = lax.rem(root - leaf + n_leaf, n_leaf) - 1

    def seen_copy(block, slot):
        place = slice(0, height(block))
        return pltpu.make_async_remote_copy(
            src_ref=bulk_ref.at[block, place], dst_ref=seen_in.at[slot, SEEN.index(block), place],
            send_sem=gram_send.at[block], recv_sem=seen_recv.at[slot, SEEN.index(block)],
            device_id={"leaf": root, "top": after_top}, device_id_type=MESH,
        )

    def store(ref, block, value, symmetric):
        if symmetric:
            ref[block, :packed] = pack(value)
        else:
            ref[block] = value

    def piece_copy(block, number):
        a, b = peers[number]
        count, rows = parts(block), r // parts(block)
        there = beside(a, b)
        index = there["mid"] if count == n_mid else there["mid"] * n_top + there["top"]
        return pltpu.make_async_remote_copy(
            src_ref=raw_ref.at[PIECES.index(block), pl.ds(pl.multiple_of(index * rows, PANEL), rows)],
            dst_ref=piece_in.at[number, PIECES.index(block), slice(0, rows)],
            send_sem=piece_send.at[number, PIECES.index(block)], recv_sem=piece_recv.at[number, PIECES.index(block)],
            device_id=there, device_id_type=MESH,
        )

    def sharers(block):
        return [k for k, (a, b) in enumerate(peers) if b == 0 or parts(block) != n_mid]

    def own_place(block, group):
        rows = r // parts(block)
        index = mid if parts(block) == n_mid else mid * n_top + group
        return pl.ds(pl.multiple_of(index * rows, PANEL), rows)

    def share(block, value):
        raw_ref[PIECES.index(block)] = value
        for number in sharers(block):
            piece_copy(block, number).start()

    def join(block):
        k = PIECES.index(block)
        total = raw_ref[k, own_place(block, top)]
        for number in sharers(block):
            piece_copy(block, number).wait_recv()
            total = total + piece_in[number, k, : r // parts(block)]
        bulk_ref[block, : r // parts(block)] = total

    def give(block, value):
        store(bulk_ref, block, value, block in SYMMETRIC)

        if block not in LATER:
            @pl.when(is_other)
            def _():
                gram_copy(block, slot_here).start()

    prec, fine = fetch(0), fetch(1)
    solved_f = dot(prec, fine)
    s_ref[0] = solved_f
    gram_ff = dot(fine.T, solved_f)
    meet()
    give(FF, gram_ff)
    middle = fetch(2)
    mid_t = middle.T
    give(MF, dot(mid_t, solved_f))
    solved_m = dot(prec, middle)
    s_ref[1] = solved_m
    give(MM, dot(mid_t, solved_m))
    coarse = fetch(3)
    coarse_t = coarse.T
    give(CF, dot(coarse_t, solved_f))
    share(CM, dot(coarse_t, solved_m))
    solved_c = dot(prec, coarse)
    s_ref[2] = solved_c
    share(CC, dot(coarse_t, solved_c))
    obs = fetch(4)
    obs_t = obs.T
    share(YM, dot(obs_t, solved_m))
    share(YC, dot(obs_t, solved_c))
    give(YF, dot(obs_t, solved_f))
    s_ref[3] = dot(prec, obs)
    for k in range(5, 8):
        loads[k].wait()

    def gathered(block):
        place = slice(0, height(block))
        if block in PIECES:
            join(block)
        total = bulk_ref[block, place]
        for slot in range(n_leaf - 1):
            gram_copy(block, slot).wait_recv()
            total = total + gram_in[slot, block, place]
        return total

    def down_copy(block, slot, target):
        return pltpu.make_async_remote_copy(
            src_ref=down_ref.at[block], dst_ref=down_ref.at[block],
            send_sem=down_send.at[block, slot], recv_sem=down_recv.at[block],
            device_id={"leaf": target}, device_id_type=MESH,
        )

    def send_down(block, value):
        down_ref[block] = value
        for slot, exists in enumerate((root > 0, root < n_leaf - 1)):
            def go():
                down_copy(block, slot, root + 2 * slot - 1).start()

            if n_leaf > 2:
                go()
            else:
                pl.when(exists)(go)

    def spread_copy(block, step):
        return pltpu.make_async_remote_copy(
            src_ref=down_ref.at[block], dst_ref=down_ref.at[block],
            send_sem=spread_send.at[block - 3, step - 1], recv_sem=down_recv.at[block],
            device_id=leaf_at(step), device_id_type=MESH,
        )

    def send_all(block, value):
        down_ref[block] = value
        for step in leaf_steps:
            spread_copy(block, step).start()

    def pass_on(block):
        down_copy(block, 0, outer).wait_recv()
        down_copy(block, 0, outer).start()

    def seen(block):
        place = slice(0, height(block))
        for slot in range(n_leaf):
            seen_copy(block, slot).wait_recv()
        total = seen_in[0, SEEN.index(block), place]
        for slot in range(1, n_leaf):
            total = total + seen_in[slot, SEEN.index(block), place]
        return total

    def help_copy(number):
        return pltpu.make_async_remote_copy(
            src_ref=kept_ref.at[number], dst_ref=kept_ref.at[number],
            send_sem=help_send.at[number], recv_sem=help_recv.at[number],
            device_id={"top": after_top}, device_id_type=MESH,
        )

    def keep(number, value):
        kept_ref[number] = value
        help_copy(number).start()

    def answer_copy(number, step):
        target, arrival = (
            (down_ref.at[2], down_recv.at[2]),
            (last_ref.at[before_top, 1], last_recv.at[1, before_top]),
            (down_ref.at[4], down_recv.at[4]),
        )[number]
        return pltpu.make_async_remote_copy(
            src_ref=answer_ref.at[number], dst_ref=target,
            send_sem=answer_send.at[number, step], recv_sem=arrival,
            device_id={**leaf_at(step), "top": before_top}, device_id_type=MESH,
        )

    def send_answer(number, value):
        answer_ref[number] = value
        for step in [*leaf_steps, 0]:
            answer_copy(number, step).start()

    def cross_place(block):
        return slice(0, packed if block in (0, 3) else r)

    def cross_copy(block, step):
        return pltpu.make_async_remote_copy(
            src_ref=cross_ref.at[block, cross_place(block)], dst_ref=cross_in.at[step - 1, block, cross_place(block)],
            send_sem=cross_send.at[block, step - 1], recv_sem=cross_recv.at[block, step - 1],
            device_id={"mid": lax.rem(mid + step, n_mid)}, device_id_type=MESH,
        )

    def cross_start(block):
        for step in range(1, n_mid):
            cross_copy(block, step).start()

    def crossed(block):
        total = cross_ref[block, cross_place(block)]
        for step in range(1, n_mid):
            cross_copy(block, step).wait_recv()
            total = total + cross_in[step - 1, block, cross_place(block)]
        return total

    def corrected(raw, value):
        total_ref[...] = value
        piece, group = (seen(raw), before_top) if raw in SEEN else (gathered(raw), top)
        total_ref[own_place(raw, group)] = total_ref[own_place(raw, group)] + piece
        return total_ref[...]

    def last_place(block):
        return slice(0, r if block else packed)

    def last_copy(block, step):
        return pltpu.make_async_remote_copy(
            src_ref=last_ref.at[top, block, last_place(block)], dst_ref=last_ref.at[top, block, last_place(block)],
            send_sem=last_send.at[block, step - 1], recv_sem=last_recv.at[block, top],
            device_id=leaf_at(step), device_id_type=MESH,
        )

    def swap_copy(block, source, step):
        return pltpu.make_async_remote_copy(
            src_ref=last_ref.at[source, block, last_place(block)], dst_ref=last_ref.at[source, block, last_place(block)],
            send_sem=swap_send.at[block, step - 1], recv_sem=last_recv.at[block, source],
            device_id={"top": lax.rem(top + step, n_top)}, device_id_type=MESH,
        )

    def swap(block):
        for step in range(1, n_top):
            swap_copy(block, top, step).start()

    def send_last(block):
        for step in leaf_steps:
            last_copy(block, step).start()
        swap(block)

    def after_fine():
        s_ref[1] = s_ref[1] + dot_nt(s_ref[0], down_ref[0])
        s_ref[2] = s_ref[2] + dot_nt(s_ref[0], down_ref[1])
        s_ref[3] = s_ref[3] + dot_nt(s_ref[0], down_ref[2])

    @pl.when(is_root)
    def _():
        inverse = negated_inverse(a_ref, in_ref[5] + unpack(gathered(FF)))
        mf = gathered(MF)
        n_m = dot(mf, inverse)
        store(cross_ref, 0, unpack(gathered(MM)) + dot_nt(n_m, mf), True)
        cross_start(0)
        send_down(0, n_m)
        keep(0, inverse)
        keep(1, mf)
        cf = gathered(CF)
        n_c = dot(cf, inverse)
        keep(2, cf)
        lost = dot_nt(n_c, kept_ref[1:3].reshape(2 * r, r))
        cross_ref[1] = corrected(CM, lost[:, :r])
        cross_start(1)
        store(cross_ref, 3, corrected(CC, lost[:, r:]), True)
        cross_start(3)
        send_down(1, n_c)
        for block in SEEN:
            if block in PIECES:
                join(block)
            seen_copy(block, 0).start()

        inverse = negated_inverse(a_ref, in_ref[6] + unpack(crossed(0)))
        cm = crossed(1)
        q_c = dot(cm, inverse)
        store(last_ref.at[top], 0, unpack(crossed(3)) + dot_nt(q_c, cm), True)
        send_last(0)
        keep(3, inverse)
        keep(4, cm)
        send_all(3, q_c)

    @pl.when(is_other)
    def _():
        for block in LATER:
            if block in PIECES:
                join(block)
            if block in SEEN:
                seen_copy(block, slot_here + 1).start()
            else:
                gram_copy(block, slot_here).start()

    @pl.when(has_outer)
    def _():
        pass_on(0)

    @pl.when(is_helper)
    def _():
        for number in range(2):
            help_copy(number).wait_recv()
        n_y = dot(seen(YF), kept_ref[0])
        send_answer(0, n_y)
        help_copy(2).wait_recv()
        lost = dot_nt(n_y, kept_ref[1:3].reshape(2 * r, r))
        cross_ref[2] = corrected(YM, lost[:, :r])
        cross_start(2)
        cross_ref[4] = corrected(YC, lost[:, r:])
        cross_start(4)

    @pl.when(has_outer)
    def _():
        pass_on(1)

    @pl.when(is_helper)
    def _():
        for number in range(3, 5):
            help_copy(number).wait_recv()
        q_y = dot(crossed(2), kept_ref[3])
        send_answer(1, crossed(4) + dot_nt(q_y, kept_ref[4]))
        send_answer(2, q_y)

    @pl.when(is_other)
    def _():
        last_copy(0, 1).wait_recv()
        swap(0)

    @pl.when(is_other & ((outer < 0) | (outer >= n_leaf)))
    def _():
        down_copy(0, 0, root).wait_recv()
        down_copy(1, 0, root).wait_recv()

    down_copy(2, 0, root).wait_recv()
    after_fine()

    def others_arrived(block):
        for step in range(1, n_top):
            swap_copy(block, lax.rem(top + step, n_top), step).wait_recv()

    others_arrived(0)
    coarse_sum = last_ref[0, 0, :packed]
    for t in range(1, n_top):
        coarse_sum = coarse_sum + last_ref[t, 0, :packed]

    def middle_of_inverse():
        last_copy(1, 1).wait_recv()
        swap(1)

    inverse = negated_inverse(a_ref, in_ref[7] + unpack(coarse_sum), middle_of_inverse)

    @pl.when(is_other)
    def _():
        spread_copy(3, 1).wait_recv()

    spread_copy(4, 1).wait_recv()
    others_arrived(1)
    right = last_ref[0, 1]
    for t in range(1, n_top):
        right = right + last_ref[t, 1]
    after = dot_nt(s_ref[1], down_ref[3:5].reshape(2 * r, r))
    out_ref[...] = s_ref[3] + after[:, r:] + dot_nt(s_ref[2] + after[:, :r], dot(right, inverse))

    for block in PIECES:
        for number in sharers(block):
            piece_copy(block, number).wait_send()
    for block in range(2):
        for step in range(1, n_top):
            swap_copy(block, top, step).wait_send()

    @pl.when(is_root)
    def _():
        for block in (0, 1, 3):
            for step in range(1, n_mid):
                cross_copy(block, step).wait_send()
        for step in leaf_steps:
            spread_copy(3, step).wait_send()
            last_copy(0, step).wait_send()
        for number in range(5):
            help_copy(number).wait_send()
        for block in SEEN:
            seen_copy(block, 0).wait_send()
        for block in range(2):
            for slot, exists in enumerate((root > 0, root < n_leaf - 1)):
                def done():
                    down_copy(block, slot, root + 2 * slot - 1).wait_send()

                if n_leaf > 2:
                    done()
                else:
                    pl.when(exists)(done)

    @pl.when(is_helper)
    def _():
        for block in (2, 4):
            for step in range(1, n_mid):
                cross_copy(block, step).wait_send()
        for number in range(3):
            for step in range(n_leaf):
                answer_copy(number, step).wait_send()

    @pl.when(is_other)
    def _():
        for block in range(9):
            gram_copy(block, slot_here).wait_send()

    @pl.when(has_outer)
    def _():
        for block in range(2):
            down_copy(block, 0, outer).wait_send()


def local(n_leaf, n_mid, n_top, *operands):
    blocks = [x.reshape(x.shape[-2:]) for x in operands]
    r = blocks[1].shape[1]
    f32 = jnp.float32
    dma = pltpu.SemaphoreType.DMA
    beside = max(n_mid * n_top - 1, 1)
    answer = pl.pallas_call(
        functools.partial(kernel, n_leaf, n_mid, n_top),
        out_shape=jax.ShapeDtypeStruct(blocks[-1].shape, f32),
        in_specs=[pl.BlockSpec(memory_space=pl.ANY)] * len(blocks),
        out_specs=pl.BlockSpec(memory_space=pltpu.VMEM),
        scratch_shapes=[
            pltpu.VMEM((8, r, r), f32),
            pltpu.VMEM((r + 2 * PANEL, r), f32),
            pltpu.VMEM((4, r, r), f32),
            pltpu.VMEM((4, r, r), f32),
            pltpu.VMEM((9, r, r), f32),
            pltpu.VMEM((beside, 4, r // n_mid, r), f32),
            pltpu.VMEM((n_leaf - 1, 9, r, r), f32),
            pltpu.VMEM((r, r), f32),
            pltpu.VMEM((5, r, r), f32),
            pltpu.VMEM((5, r, r), f32),
            pltpu.VMEM((5, r, r), f32),
            pltpu.VMEM((n_mid - 1, 5, r, r), f32),
            pltpu.VMEM((n_top, 2, r, r), f32),
            pltpu.VMEM((n_leaf, 3, r, r), f32),
            pltpu.VMEM((3, r, r), f32),
            dma((8,)),
            dma((beside, 4)), dma((beside, 4)),
            dma((9,)), dma((n_leaf - 1, 9)),
            dma((3, 2)), dma((5,)), dma((2, n_leaf - 1)),
            dma((5, n_mid - 1)), dma((5, n_mid - 1)),
            dma((2, n_leaf - 1)), dma((2, n_top)), dma((2, n_top - 1)),
            dma((n_leaf, 3)), dma((5,)), dma((5,)), dma((3, n_leaf)),
        ],
        compiler_params=pltpu.CompilerParams(
            collective_id=0, has_side_effects=True, vmem_limit_bytes=VMEM_ROOM - 3 * r * blocks[-1].shape[1] * 2,
        ),
    )(*blocks)
    return answer[None, None, None]


def solution(mesh):
    spread = P(("parts", "leaf"), "mid", "top", None, None)
    sizes = (mesh.shape["leaf"], mesh.shape["mid"], mesh.shape["top"])
    return jax.shard_map(
        functools.partial(local, *sizes),
        mesh=mesh,
        in_specs=(spread, spread, spread, spread, P(), P(), P(), spread),
        out_specs=spread,
        check_vma=False,
    )
```

```python
import functools

import jax
import jax.numpy as jnp
from jax import lax
from jax.experimental import pallas as pl
from jax.experimental.pallas import tpu as pltpu
from jax.sharding import PartitionSpec as P

MESH = pl.DeviceIdType.MESH
PANEL = 8
VMEM_ROOM = 56_558_000


def dot(left_hand, right_side):
    return jnp.dot(
        left_hand, right_side, precision=lax.Precision.HIGHEST, preferred_element_type=jnp.float32
    )


def split3(x):
    high = x.astype(jnp.bfloat16).astype(jnp.float32)
    rest = x - high
    mid = rest.astype(jnp.bfloat16).astype(jnp.float32)
    low = (rest - mid).astype(jnp.bfloat16).astype(jnp.float32)
    return high, mid, low


def spread_panel(panel):
    p1, p2, p3 = split3(panel)
    return jnp.concatenate([p1, p1, p2, p2, p1, p3], axis=0).T.astype(jnp.bfloat16)


def rank_update(spread, scaled):
    r1, r2, r3 = split3(scaled)
    right_side = jnp.concatenate([r1, r2, r1, r2, r3, r1], axis=0).astype(jnp.bfloat16)
    return jnp.dot(spread, right_side, preferred_element_type=jnp.float32)


def negated_inverse(a_ref, matrix, between=None):
    size = matrix.shape[0]
    zero = jnp.zeros((PANEL, size), jnp.float32)
    a_ref[pl.ds(0, PANEL), :] = zero
    a_ref[pl.ds(PANEL, size), :] = matrix
    a_ref[pl.ds(PANEL + size, PANEL), :] = zero
    lane = lax.broadcasted_iota(jnp.int32, (PANEL, size), 1)
    sub = lax.broadcasted_iota(jnp.int32, (PANEL, size), 0)
    lane_full = lax.broadcasted_iota(jnp.int32, (size, size), 1)

    def lanes(block, index):
        picked = jnp.where(lane == index, block, 0.0)
        return jnp.broadcast_to(jnp.sum(picked, axis=1, keepdims=True), block.shape)

    def row_of(block, i):
        return jnp.broadcast_to(block[i : i + 1], block.shape)

    def apply(k, spread, scaled):
        inside = (lane_full >= k * PANEL) & (lane_full < (k + 1) * PANEL)
        current = a_ref[pl.ds(PANEL, size), :]
        a_ref[pl.ds(PANEL, size), :] = jnp.where(inside, 0.0, current) - rank_update(spread, scaled)
        a_ref[pl.ds(pl.multiple_of((k + 1) * PANEL, PANEL), PANEL), :] = scaled

    def body(k, carry):
        spread_before, scaled_before, panel = carry
        apply(k - 1, spread_before, scaled_before)
        inside = (lane >= k * PANEL) & (lane < (k + 1) * PANEL)
        cols = [lanes(panel, k * PANEL + j) for j in range(PANEL)]
        ahead = (k + 1) * PANEL + sub
        below = [lanes(row_of(panel, j), ahead) for j in range(PANEL)]
        spread = spread_panel(panel)
        following = a_ref[pl.ds(pl.multiple_of((k + 2) * PANEL, PANEL), PANEL), :]
        x = jnp.where(inside, jnp.where(lane - k * PANEL == sub, 1.0, 0.0), panel)
        gone = jnp.zeros_like(x)
        scale = gone
        for i in range(PANEL):
            pivot = 1.0 / row_of(cols[i], i)
            here = sub == i
            factor = jnp.where(here, 0.0, cols[i])
            row = row_of(x, i)
            across, down = factor * pivot, below[i] * pivot
            for j in range(i + 1, PANEL):
                entry = row_of(cols[j], i)
                if j == i + 1:
                    cols[j] = cols[j] - (factor * entry) * pivot
                else:
                    cols[j] = cols[j] - across * entry
                below[j] = below[j] - down * entry
            x = x - across * row
            gone = gone + down * row
            scale = jnp.where(here, pivot, scale)
        x = x * scale
        return spread, jnp.where(inside, -x, x), jnp.where(inside, gone, following - gone)

    steps = size // PANEL
    carry = (spread_panel(zero), zero, matrix[:PANEL])
    if between is None:
        spread, scaled, _ = lax.fori_loop(0, steps, body, carry)
    else:
        carry = lax.fori_loop(0, steps // 2, body, carry)
        between()
        spread, scaled, _ = lax.fori_loop(steps // 2, steps, body, carry)
    apply(steps - 1, spread, scaled)
    return a_ref[pl.ds(PANEL, size), :]


def dot_nt(left_hand, right_rows):
    return lax.dot_general(
        left_hand, right_rows, (((1,), (1,)), ((), ())),
        precision=lax.Precision.HIGHEST, preferred_element_type=jnp.float32,
    )


def pack(matrix):
    half, size = matrix.shape[0] // 2, matrix.shape[1]
    lane = lax.broadcasted_iota(jnp.int32, (PANEL, size), 1)
    blocks = [matrix[:PANEL]]
    for start in range(PANEL, half + 1, PANEL):
        moved = pltpu.roll(matrix[size - start : size - start + PANEL], start, 1)
        blocks.append(moved if start == half else jnp.where(lane < start, moved, matrix[start : start + PANEL]))
    return jnp.concatenate(blocks, axis=0)


def unpack(packed):
    half, size = packed.shape[0] - PANEL, packed.shape[1]
    bottom = [pltpu.roll(packed[start : start + PANEL], size - start, 1) for start in range(half, 0, -PANEL)]
    return jnp.concatenate([packed[:half], *bottom], axis=0)


FF, MF, MM, CF, CM, YF, YM, CC, YC = range(9)
SYMMETRIC = (FF, MM)
LATER = (CM, CC, YF, YM, YC)
PIECES = (CM, YM, CC, YC)
SEEN = (YF, YM, YC)


def kernel(
    n_leaf, n_mid, n_top,
    prec_hbm, fine_hbm, mid_hbm, coarse_hbm, core_fine_hbm, core_mid_hbm, core_coarse_hbm, obs_hbm,
    out_ref,
    in_ref, a_ref, s_ref, raw_ref, bulk_ref, piece_in, gram_in, total_ref, kept_ref, down_ref, cross_ref, cross_in, last_ref, seen_in, answer_ref,
    in_sem, piece_send, piece_recv, gram_send, gram_recv, down_send, down_recv, spread_send,
    cross_send, cross_recv, last_send, last_recv, swap_send, seen_recv, help_send, help_recv, answer_send,
):
    r = bulk_ref.shape[1]
    packed = r // 2 + PANEL
    leaf, mid, top = lax.axis_index("leaf"), lax.axis_index("mid"), lax.axis_index("top")
    low, high = (n_leaf - 1) // 2, n_leaf // 2

    def root_of(index):
        return low + lax.rem(index, 2) * (high - low)

    root = root_of(top)
    after_top, before_top = lax.rem(top + 1, n_top), lax.rem(top + n_top - 1, n_top)
    is_helper = leaf == root_of(before_top)
    is_root = leaf == root
    is_other = leaf != root
    side = (leaf > root).astype(jnp.int32)
    inner, outer = leaf + 1 - 2 * side, leaf - 1 + 2 * side
    has_outer = is_other & (outer >= 0) & (outer < n_leaf)
    inner_is_other = is_other & (inner != root)
    barrier = pltpu.get_barrier_semaphore()

    def greet(device):
        pl.semaphore_signal(barrier, inc=1, device_id=device, device_id_type=MESH)

    leaf_steps = sorted(range(1, n_leaf), key=lambda step: (abs(2 * step - n_leaf), step))
    peers = [(a, b) for a in range(n_mid) for b in range(n_top) if (a, b) != (0, 0)]

    def beside(a, b):
        return {"mid": lax.rem(mid + a, n_mid), "top": lax.rem(top + b, n_top)}

    def leaf_at(step):
        return {"leaf": lax.rem(leaf + step, n_leaf)}

    for a, b in peers:
        greet(beside(a, b))

    @pl.when(is_root)
    def _():
        for step in leaf_steps:
            greet(leaf_at(step))

    @pl.when(is_other)
    def _():
        greet({"leaf": root})

        greet({"leaf": root, "top": after_top})

    @pl.when(is_helper)
    def _():
        for step in leaf_steps:
            greet({**leaf_at(step), "top": before_top})

    @pl.when(has_outer)
    def _():
        greet({"leaf": outer})

    @pl.when(inner_is_other)
    def _():
        greet({"leaf": inner})

    sources = [prec_hbm, fine_hbm, mid_hbm, coarse_hbm, obs_hbm, core_fine_hbm, core_mid_hbm, core_coarse_hbm]
    loads = [pltpu.make_async_copy(src, in_ref.at[k], in_sem.at[k]) for k, src in enumerate(sources)]
    for load in loads:
        load.start()

    def fetch(k):
        loads[k].wait()
        return in_ref[k]

    def meet():
        around = jnp.where(is_root, n_leaf - 1, 2 + has_outer.astype(jnp.int32) + inner_is_other.astype(jnp.int32))
        helped = jnp.where(is_helper, n_leaf - 1, 0)
        pl.semaphore_wait(barrier, len(peers) + around + helped)

    def parts(block):
        return n_mid if block in (CM, YM) else n_mid * n_top

    def height(block):
        if block in SYMMETRIC:
            return packed
        return r // parts(block) if block in PIECES else r

    def gram_copy(block, slot):
        place = slice(0, height(block))
        return pltpu.make_async_remote_copy(
            src_ref=bulk_ref.at[block, place], dst_ref=gram_in.at[slot, block, place],
            send_sem=gram_send.at[block], recv_sem=gram_recv.at[slot, block],
            device_id={"leaf": root}, device_id_type=MESH,
        )

    slot_here = lax.rem(root - leaf + n_leaf, n_leaf) - 1

    def seen_copy(block, slot):
        place = slice(0, height(block))
        return pltpu.make_async_remote_copy(
            src_ref=bulk_ref.at[block, place], dst_ref=seen_in.at[slot, SEEN.index(block), place],
            send_sem=gram_send.at[block], recv_sem=seen_recv.at[slot, SEEN.index(block)],
            device_id={"leaf": root, "top": after_top}, device_id_type=MESH,
        )

    def store(ref, block, value, symmetric):
        if symmetric:
            ref[block, :packed] = pack(value)
        else:
            ref[block] = value

    def piece_copy(block, number):
        a, b = peers[number]
        count, rows = parts(block), r // parts(block)
        there = beside(a, b)
        index = there["mid"] if count == n_mid else there["mid"] * n_top + there["top"]
        return pltpu.make_async_remote_copy(
            src_ref=raw_ref.at[PIECES.index(block), pl.ds(pl.multiple_of(index * rows, PANEL), rows)],
            dst_ref=piece_in.at[number, PIECES.index(block), slice(0, rows)],
            send_sem=piece_send.at[number, PIECES.index(block)], recv_sem=piece_recv.at[number, PIECES.index(block)],
            device_id=there, device_id_type=MESH,
        )

    def sharers(block):
        return [k for k, (a, b) in enumerate(peers) if b == 0 or parts(block) != n_mid]

    def own_place(block, group):
        rows = r // parts(block)
        index = mid if parts(block) == n_mid else mid * n_top + group
        return pl.ds(pl.multiple_of(index * rows, PANEL), rows)

    def share(block, value):
        raw_ref[PIECES.index(block)] = value
        for number in sharers(block):
            piece_copy(block, number).start()

    def join(block):
        k = PIECES.index(block)
        total = raw_ref[k, own_place(block, top)]
        for number in sharers(block):
            piece_copy(block, number).wait_recv()
            total = total + piece_in[number, k, : r // parts(block)]
        bulk_ref[block, : r // parts(block)] = total

    def give(block, value):
        store(bulk_ref, block, value, block in SYMMETRIC)

        if block not in LATER:
            @pl.when(is_other)
            def _():
                gram_copy(block, slot_here).start()

    prec, fine = fetch(0), fetch(1)
    solved_f = dot(prec, fine)
    s_ref[0] = solved_f
    gram_ff = dot(fine.T, solved_f)
    meet()
    give(FF, gram_ff)
    middle = fetch(2)
    mid_t = middle.T
    give(MF, dot(mid_t, solved_f))
    solved_m = dot(prec, middle)
    s_ref[1] = solved_m
    give(MM, dot(mid_t, solved_m))
    coarse = fetch(3)
    coarse_t = coarse.T
    give(CF, dot(coarse_t, solved_f))
    share(CM, dot(coarse_t, solved_m))
    solved_c = dot(prec, coarse)
    s_ref[2] = solved_c
    share(CC, dot(coarse_t, solved_c))
    obs = fetch(4)
    obs_t = obs.T
    share(YM, dot(obs_t, solved_m))
    share(YC, dot(obs_t, solved_c))
    give(YF, dot(obs_t, solved_f))
    s_ref[3] = dot(prec, obs)
    for k in range(5, 8):
        loads[k].wait()

    def gathered(block):
        place = slice(0, height(block))
        if block in PIECES:
            join(block)
        total = bulk_ref[block, place]
        for slot in range(n_leaf - 1):
            gram_copy(block, slot).wait_recv()
            total = total + gram_in[slot, block, place]
        return total

    def down_copy(block, slot, target):
        return pltpu.make_async_remote_copy(
            src_ref=down_ref.at[block], dst_ref=down_ref.at[block],
            send_sem=down_send.at[block, slot], recv_sem=down_recv.at[block],
            device_id={"leaf": target}, device_id_type=MESH,
        )

    def send_down(block, value):
        down_ref[block] = value
        for slot, exists in enumerate((root > 0, root < n_leaf - 1)):
            def go():
                down_copy(block, slot, root + 2 * slot - 1).start()

            if n_leaf > 2:
                go()
            else:
                pl.when(exists)(go)

    def spread_copy(block, step):
        return pltpu.make_async_remote_copy(
            src_ref=down_ref.at[block], dst_ref=down_ref.at[block],
            send_sem=spread_send.at[block - 3, step - 1], recv_sem=down_recv.at[block],
            device_id=leaf_at(step), device_id_type=MESH,
        )

    def send_all(block, value):
        down_ref[block] = value
        for step in leaf_steps:
            spread_copy(block, step).start()

    def pass_on(block):
        down_copy(block, 0, outer).wait_recv()
        down_copy(block, 0, outer).start()

    def seen(block):
        place = slice(0, height(block))
        for slot in range(n_leaf):
            seen_copy(block, slot).wait_recv()
        total = seen_in[0, SEEN.index(block), place]
        for slot in range(1, n_leaf):
            total = total + seen_in[slot, SEEN.index(block), place]
        return total

    def help_copy(number):
        return pltpu.make_async_remote_copy(
            src_ref=kept_ref.at[number], dst_ref=kept_ref.at[number],
            send_sem=help_send.at[number], recv_sem=help_recv.at[number],
            device_id={"top": after_top}, device_id_type=MESH,
        )

    def keep(number, value):
        kept_ref[number] = value
        help_copy(number).start()

    def answer_copy(number, step):
        target, arrival = (
            (down_ref.at[2], down_recv.at[2]),
            (last_ref.at[before_top, 1], last_recv.at[1, before_top]),
            (down_ref.at[4], down_recv.at[4]),
        )[number]
        return pltpu.make_async_remote_copy(
            src_ref=answer_ref.at[number], dst_ref=target,
            send_sem=answer_send.at[number, step], recv_sem=arrival,
            device_id={**leaf_at(step), "top": before_top}, device_id_type=MESH,
        )

    def send_answer(number, value):
        answer_ref[number] = value
        for step in [*leaf_steps, 0]:
            answer_copy(number, step).start()

    def cross_place(block):
        return slice(0, packed if block in (0, 3) else r)

    def cross_copy(block, step):
        return pltpu.make_async_remote_copy(
            src_ref=cross_ref.at[block, cross_place(block)], dst_ref=cross_in.at[step - 1, block, cross_place(block)],
            send_sem=cross_send.at[block, step - 1], recv_sem=cross_recv.at[block, step - 1],
            device_id={"mid": lax.rem(mid + step, n_mid)}, device_id_type=MESH,
        )

    def cross_start(block):
        for step in range(1, n_mid):
            cross_copy(block, step).start()

    def crossed(block):
        total = cross_ref[block, cross_place(block)]
        for step in range(1, n_mid):
            cross_copy(block, step).wait_recv()
            total = total + cross_in[step - 1, block, cross_place(block)]
        return total

    def corrected(raw, value):
        total_ref[...] = value
        piece, group = (seen(raw), before_top) if raw in SEEN else (gathered(raw), top)
        total_ref[own_place(raw, group)] = total_ref[own_place(raw, group)] + piece
        return total_ref[...]

    def last_place(block):
        return slice(0, r if block else packed)

    def last_copy(block, step):
        return pltpu.make_async_remote_copy(
            src_ref=last_ref.at[top, block, last_place(block)], dst_ref=last_ref.at[top, block, last_place(block)],
            send_sem=last_send.at[block, step - 1], recv_sem=last_recv.at[block, top],
            device_id=leaf_at(step), device_id_type=MESH,
        )

    def swap_copy(block, source, step):
        return pltpu.make_async_remote_copy(
            src_ref=last_ref.at[source, block, last_place(block)], dst_ref=last_ref.at[source, block, last_place(block)],
            send_sem=swap_send.at[block, step - 1], recv_sem=last_recv.at[block, source],
            device_id={"top": lax.rem(top + step, n_top)}, device_id_type=MESH,
        )

    def swap(block):
        for step in range(1, n_top):
            swap_copy(block, top, step).start()

    def send_last(block):
        for step in leaf_steps:
            last_copy(block, step).start()
        swap(block)

    def after_fine():
        s_ref[1] = s_ref[1] + dot_nt(s_ref[0], down_ref[0])
        s_ref[2] = s_ref[2] + dot_nt(s_ref[0], down_ref[1])
        s_ref[3] = s_ref[3] + dot_nt(s_ref[0], down_ref[2])

    @pl.when(is_root)
    def _():
        inverse = negated_inverse(a_ref, in_ref[5] + unpack(gathered(FF)))
        keep(0, inverse)
        mf = gathered(MF)
        keep(1, mf)
        n_m = dot(mf, inverse)
        store(cross_ref, 0, unpack(gathered(MM)) + dot_nt(n_m, mf), True)
        cross_start(0)
        send_down(0, n_m)
        cf = gathered(CF)
        n_c = dot(cf, inverse)
        keep(2, cf)
        lost = dot_nt(n_c, kept_ref[1:3].reshape(2 * r, r))
        cross_ref[1] = corrected(CM, lost[:, :r])
        cross_start(1)
        store(cross_ref, 3, corrected(CC, lost[:, r:]), True)
        cross_start(3)
        send_down(1, n_c)
        for block in SEEN:
            if block in PIECES:
                join(block)
            seen_copy(block, 0).start()

        inverse = negated_inverse(a_ref, in_ref[6] + unpack(crossed(0)))
        keep(3, inverse)
        cm = crossed(1)
        keep(4, cm)
        q_c = dot(cm, inverse)
        store(last_ref.at[top], 0, unpack(crossed(3)) + dot_nt(q_c, cm), True)
        send_last(0)
        send_all(3, q_c)

    @pl.when(is_other)
    def _():
        for block in LATER:
            if block in PIECES:
                join(block)
            if block in SEEN:
                seen_copy(block, slot_here + 1).start()
            else:
                gram_copy(block, slot_here).start()

    @pl.when(has_outer)
    def _():
        pass_on(0)

    @pl.when(is_helper)
    def _():
        for number in range(2):
            help_copy(number).wait_recv()
        n_y = dot(seen(YF), kept_ref[0])
        send_answer(0, n_y)
        help_copy(2).wait_recv()
        lost = dot_nt(n_y, kept_ref[1:3].reshape(2 * r, r))
        cross_ref[2] = corrected(YM, lost[:, :r])
        cross_start(2)
        cross_ref[4] = corrected(YC, lost[:, r:])
        cross_start(4)

    @pl.when(has_outer)
    def _():
        pass_on(1)

    @pl.when(is_helper)
    def _():
        for number in range(3, 5):
            help_copy(number).wait_recv()
        q_y = dot(crossed(2), kept_ref[3])
        send_answer(1, crossed(4) + dot_nt(q_y, kept_ref[4]))
        send_answer(2, q_y)

    @pl.when(is_other)
    def _():
        last_copy(0, 1).wait_recv()
        swap(0)

    @pl.when(is_other & ((outer < 0) | (outer >= n_leaf)))
    def _():
        down_copy(0, 0, root).wait_recv()
        down_copy(1, 0, root).wait_recv()

    down_copy(2, 0, root).wait_recv()
    after_fine()

    def others_arrived(block):
        for step in range(1, n_top):
            swap_copy(block, lax.rem(top + step, n_top), step).wait_recv()

    others_arrived(0)
    coarse_sum = last_ref[0, 0, :packed]
    for t in range(1, n_top):
        coarse_sum = coarse_sum + last_ref[t, 0, :packed]

    def middle_of_inverse():
        last_copy(1, 1).wait_recv()
        swap(1)

    inverse = negated_inverse(a_ref, in_ref[7] + unpack(coarse_sum), middle_of_inverse)

    @pl.when(is_other)
    def _():
        spread_copy(3, 1).wait_recv()

    spread_copy(4, 1).wait_recv()
    others_arrived(1)
    right = last_ref[0, 1]
    for t in range(1, n_top):
        right = right + last_ref[t, 1]
    after = dot_nt(s_ref[1], down_ref[3:5].reshape(2 * r, r))
    out_ref[...] = s_ref[3] + after[:, r:] + dot_nt(s_ref[2] + after[:, :r], dot(right, inverse))

    for block in PIECES:
        for number in sharers(block):
            piece_copy(block, number).wait_send()
    for block in range(2):
        for step in range(1, n_top):
            swap_copy(block, top, step).wait_send()

    @pl.when(is_root)
    def _():
        for block in (0, 1, 3):
            for step in range(1, n_mid):
                cross_copy(block, step).wait_send()
        for step in leaf_steps:
            spread_copy(3, step).wait_send()
            last_copy(0, step).wait_send()
        for number in range(5):
            help_copy(number).wait_send()
        for block in SEEN:
            seen_copy(block, 0).wait_send()
        for block in range(2):
            for slot, exists in enumerate((root > 0, root < n_leaf - 1)):
                def done():
                    down_copy(block, slot, root + 2 * slot - 1).wait_send()

                if n_leaf > 2:
                    done()
                else:
                    pl.when(exists)(done)

    @pl.when(is_helper)
    def _():
        for block in (2, 4):
            for step in range(1, n_mid):
                cross_copy(block, step).wait_send()
        for number in range(3):
            for step in range(n_leaf):
                answer_copy(number, step).wait_send()

    @pl.when(is_other)
    def _():
        for block in range(9):
            gram_copy(block, slot_here).wait_send()

    @pl.when(has_outer)
    def _():
        for block in range(2):
            down_copy(block, 0, outer).wait_send()


def local(n_leaf, n_mid, n_top, *operands):
    blocks = [x.reshape(x.shape[-2:]) for x in operands]
    r = blocks[1].shape[1]
    f32 = jnp.float32
    dma = pltpu.SemaphoreType.DMA
    beside = max(n_mid * n_top - 1, 1)
    answer = pl.pallas_call(
        functools.partial(kernel, n_leaf, n_mid, n_top),
        out_shape=jax.ShapeDtypeStruct(blocks[-1].shape, f32),
        in_specs=[pl.BlockSpec(memory_space=pl.ANY)] * len(blocks),
        out_specs=pl.BlockSpec(memory_space=pltpu.VMEM),
        scratch_shapes=[
            pltpu.VMEM((8, r, r), f32),
            pltpu.VMEM((r + 2 * PANEL, r), f32),
            pltpu.VMEM((4, r, r), f32),
            pltpu.VMEM((4, r, r), f32),
            pltpu.VMEM((9, r, r), f32),
            pltpu.VMEM((beside, 4, r // n_mid, r), f32),
            pltpu.VMEM((n_leaf - 1, 9, r, r), f32),
            pltpu.VMEM((r, r), f32),
            pltpu.VMEM((5, r, r), f32),
            pltpu.VMEM((5, r, r), f32),
            pltpu.VMEM((5, r, r), f32),
            pltpu.VMEM((n_mid - 1, 5, r, r), f32),
            pltpu.VMEM((n_top, 2, r, r), f32),
            pltpu.VMEM((n_leaf, 3, r, r), f32),
            pltpu.VMEM((3, r, r), f32),
            dma((8,)),
            dma((beside, 4)), dma((beside, 4)),
            dma((9,)), dma((n_leaf - 1, 9)),
            dma((3, 2)), dma((5,)), dma((2, n_leaf - 1)),
            dma((5, n_mid - 1)), dma((5, n_mid - 1)),
            dma((2, n_leaf - 1)), dma((2, n_top)), dma((2, n_top - 1)),
            dma((n_leaf, 3)), dma((5,)), dma((5,)), dma((3, n_leaf)),
        ],
        compiler_params=pltpu.CompilerParams(
            collective_id=0, has_side_effects=True, vmem_limit_bytes=VMEM_ROOM - 3 * r * blocks[-1].shape[1] * 2,
        ),
    )(*blocks)
    return answer[None, None, None]


def solution(mesh):
    spread = P(("parts", "leaf"), "mid", "top", None, None)
    sizes = (mesh.shape["leaf"], mesh.shape["mid"], mesh.shape["top"])
    return jax.shard_map(
        functools.partial(local, *sizes),
        mesh=mesh,
        in_specs=(spread, spread, spread, spread, P(), P(), P(), spread),
        out_specs=spread,
        check_vma=False,
    )
```
